32 devices in a mesh: dp: 4 (over x, y), tp: 8 (over z, core).
Axes of the slice: x: 2, y: 2, z: 4, core: 2. Of those that a mesh axis runs over, the one named last changes fastest.
Arguments:
- residual: float32 [1024, 2048], P('dp'), parts along dimension 0
- norm_w: bfloat16 [2, 2048], replicated
- w_in: bfloat16 [2, 2048, 2, 4096], P(None, None, None, 'tp')
- conv_w: bfloat16 [2, 4, 4096], P(None, None, 'tp')
- conv_b: bfloat16 [2, 4096], P(None, 'tp')
- w_x: bfloat16 [2, 4096, 160], P(None, 'tp')
- w_dt: bfloat16 [2, 128, 4096], P(None, None, 'tp')
- b_dt: float32 [2, 4096], P(None, 'tp')
- a_log: float32 [2, 16, 4096], P(None, None, 'tp')
- d_skip: float32 [2, 4096], P(None, 'tp')
- w_out: bfloat16 [2, 4096, 2048], P(None, 'tp')
- conv_state: bfloat16 [2, 1024, 3, 4096], P(None, 'dp', None, 'tp'), parts along dimension 1
- ssm_state: float32 [2, 1024, 16, 4096], P(None, 'dp', None, 'tp'), parts along dimension 1
Outputs:
- output 1: float32 [1024, 2048], P('dp'), parts along dimension 0
- output 2: bfloat16 [2, 1024, 3, 4096], P(None, 'dp', None, 'tp'), parts along dimension 1
- output 3: float32 [2, 1024, 16, 4096], P(None, 'dp', None, 'tp'), parts along dimension 1
There are 4 independent parts. The reference program is written for one: setup_inputs(seed, part) draws one part's arguments, and reference() takes and returns one part's arrays. A program takes and returns all parts, laid end to end along the dimension named above; an argument that names none is the same for every part.
All inputs are finite; a program needn't handle non-finite values.
Results may differ from the reference program's by a relative error of at most 0.02.
Values are sent between devices in bfloat16 or wider.
A program may use at most 1 GiB of HBM per device.

```python
import math
import jax
import jax.numpy as jnp
from jax import lax

D = 2048
INNER = 4096
STATE = 16
RANK = 128
CONV = 4
LAYERS = 2
BATCH = 256


def setup_inputs(seed: int = 0, part: int = 0) -> dict:
    root_key = jax.random.key(seed)
    shared = jax.random.split(root_key, 10)
    part_keys = jax.random.split(jax.random.fold_in(root_key, part), 3)
    proj_width = RANK + 2 * STATE
    residual = jax.random.normal(part_keys[0], (BATCH, D), jnp.float32)
    norm_w = jax.random.uniform(shared[0], (LAYERS, D), jnp.float32, 0.5, 1.5).astype(jnp.bfloat16)
    w_in = (jax.random.normal(shared[1], (LAYERS, D, 2, INNER), jnp.float32) * D ** -0.5).astype(jnp.bfloat16)
    conv_w = (0.5 * jax.random.normal(shared[2], (LAYERS, CONV, INNER), jnp.float32)).astype(jnp.bfloat16)
    conv_b = (0.3 * jax.random.normal(shared[3], (LAYERS, INNER), jnp.float32)).astype(jnp.bfloat16)
    w_x = (jax.random.normal(shared[4], (LAYERS, INNER, proj_width), jnp.float32) * INNER ** -0.5).astype(jnp.bfloat16)
    w_dt = (jax.random.normal(shared[5], (LAYERS, RANK, INNER), jnp.float32) * (0.25 * RANK ** -0.5)).astype(jnp.bfloat16)
    dt_init = jnp.exp(jax.random.uniform(shared[6], (LAYERS, INNER), jnp.float32, math.log(0.05), math.log(0.25)))
    b_dt = dt_init + jnp.log(-jnp.expm1(-dt_init))
    a_log = jax.random.uniform(shared[7], (LAYERS, STATE, INNER), jnp.float32, -0.7, 0.7)
    d_skip = jax.random.uniform(shared[8], (LAYERS, INNER), jnp.float32, 0.5, 1.5)
    w_out = (jax.random.normal(shared[9], (LAYERS, INNER, D), jnp.float32) * INNER ** -0.5).astype(jnp.bfloat16)
    conv_state = jax.random.normal(part_keys[1], (LAYERS, BATCH, CONV - 1, INNER), jnp.float32).astype(jnp.bfloat16)
    ssm_state = 0.5 * jax.random.normal(part_keys[2], (LAYERS, BATCH, STATE, INNER), jnp.float32)
    return {'residual': residual, 'norm_w': norm_w, 'w_in': w_in, 'conv_w': conv_w, 'conv_b': conv_b, 'w_x': w_x, 'w_dt': w_dt, 'b_dt': b_dt, 'a_log': a_log, 'd_skip': d_skip, 'w_out': w_out, 'conv_state': conv_state, 'ssm_state': ssm_state}


def rms_norm(vector, epsilon):
    return vector * lax.rsqrt(jnp.mean(vector * vector, axis=-1, keepdims=True) + epsilon)


def mamba_layer(residual, params):
    norm_w, w_in, conv_w, conv_b, w_x, w_dt, b_dt, a_log, d_skip, w_out, conv_state, ssm_state = params
    hidden = (rms_norm(residual, 1e-5) * norm_w.astype(jnp.float32)).astype(jnp.bfloat16)
    x_part = jnp.dot(hidden, w_in[:, 0, :], preferred_element_type=jnp.float32).astype(jnp.bfloat16)
    z_part = jnp.dot(hidden, w_in[:, 1, :], preferred_element_type=jnp.float32).astype(jnp.bfloat16)
    window = jnp.concatenate([conv_state, x_part[:, None, :]], axis=1)
    conv_pre = jnp.sum(window.astype(jnp.float32) * conv_w.astype(jnp.float32)[None], axis=1) + conv_b.astype(jnp.float32)
    x_conv = jax.nn.silu(conv_pre).astype(jnp.bfloat16)
    proj_sum = jnp.dot(x_conv, w_x, preferred_element_type=jnp.float32)
    dt_low = rms_norm(proj_sum[:, :RANK], 1e-6).astype(jnp.bfloat16)
    b_vec = rms_norm(proj_sum[:, RANK:RANK + STATE], 1e-6)
    c_vec = rms_norm(proj_sum[:, RANK + STATE:], 1e-6)
    dt_val = jax.nn.softplus(jnp.dot(dt_low, w_dt, preferred_element_type=jnp.float32) + b_dt)
    x_float = x_conv.astype(jnp.float32)
    decay_fac = jnp.exp(dt_val[:, None, :] * -jnp.exp(a_log)[None])
    new_ssm = decay_fac * ssm_state + (dt_val * x_float)[:, None, :] * b_vec[:, :, None]
    y_val = jnp.sum(new_ssm * c_vec[:, :, None], axis=1) + d_skip * x_float
    gated_y = (y_val * jax.nn.silu(z_part.astype(jnp.float32))).astype(jnp.bfloat16)
    out_sum = jnp.dot(gated_y, w_out, preferred_element_type=jnp.float32)
    return residual + out_sum, (window[:, 1:, :], new_ssm)


def reference(residual, norm_w, w_in, conv_w, conv_b, w_x, w_dt, b_dt, a_log, d_skip, w_out, conv_state, ssm_state):
    resid_out, cache_new = lax.scan(mamba_layer, residual, (norm_w, w_in, conv_w, conv_b, w_x, w_dt, b_dt, a_log, d_skip, w_out, conv_state, ssm_state))
    return resid_out, cache_new[0], cache_new[1]
```

```python
import functools

import jax
import jax.numpy as jnp
from jax import lax
from jax.experimental import pallas as pl
from jax.experimental.pallas import tpu as pltpu
from jax.sharding import PartitionSpec as P

MESH = pl.DeviceIdType.MESH
LOG2E = 1.4426950408889634
F32, BF16 = jnp.float32, jnp.bfloat16

ROWS = 256
D = 2048
E = 512
N = 16
RANK = 128
PW = RANK + 2 * N
NCH = 8
CR = ROWS // NCH
HALF = D // 2
KB = 8
KD = D // KB
OFF_B, OFF_C, OFF_D, OFF_E, OFF_F = 1, 3, 5, 7, 8


def silu(v):
    return v * jax.nn.sigmoid(v)


def rms(v, axis, eps):
    return v * lax.rsqrt(jnp.mean(v * v, axis=axis, keepdims=True) + eps)


def body(
    resid_in, norm_w, w_in, conv_w, conv_b, w_xt, w_dt, b_dt, a_log, d_skip, w_out, conv_in, ssm_in,
    resid, conv_out, ssm,
    v_norm, v_convw, v_convb, v_wxt, v_wdt, v_bdt, v_alog, v_dskip,
    w_raw, w_xz, s32, v_wout, conv0,
    hid, xcb, gate, dtb, dtx, dsx, bcb, a2,
    p_half, p_sa, p_ra, p_sb, p_rb, p_full,
    own, o_sa, o_ra, o_sb, o_rb, o_sc, o_rc, tot,
    small_sem, resid_sem, win_sem, conv_sem, ssm_sem, wout_sem,
    pa_send, pa_recv, pb_send, pb_recv, pf_send, pf_recv,
    a_send, a_recv, b_send, b_recv, c_send, c_recv, t_send, t_recv, f_send, f_recv,
):
    dp = lax.axis_index("dp")
    me = lax.axis_index("tp")
    core = lax.rem(me, 2)
    z = me // 2
    is_end = (z == 0) | (z == 3)
    is_mid = (z == 1) | (z == 2)
    partner = me + 1 - 2 * core
    zodd = lax.rem(z, 2)
    zpair = me + 2 - 4 * zodd
    midpeer = (3 - z) * 2 + core

    def dev(t):
        return (dp, t)

    def remote(src, dst, ssem, rsem, target):
        return pltpu.make_async_remote_copy(
            src_ref=src, dst_ref=dst, send_sem=ssem, recv_sem=rsem, device_id=dev(target), device_id_type=MESH)

    barrier = pltpu.get_barrier_semaphore()
    pl.semaphore_signal(barrier, inc=1, device_id=dev(partner), device_id_type=MESH)
    for k in range(1, 4):
        pl.semaphore_signal(barrier, inc=1, device_id=dev(lax.rem(me + 2 * k, 8)), device_id_type=MESH)

    copies = {}

    def load(key, src, dst, sem):
        c = pltpu.make_async_copy(src, dst, sem)
        c.start()
        copies[key] = c

    load("norm", norm_w, v_norm, small_sem.at[0])
    load("resid", resid_in, resid, resid_sem)
    for kb in range(KB):
        load(("win", 0, kb), w_in.at[0, pl.ds(kb * KD, KD)], w_raw.at[0, pl.ds(kb * KD, KD)], win_sem.at[0, kb])
    small = ((conv_w, v_convw), (conv_b, v_convb), (w_xt, v_wxt), (w_dt, v_wdt), (b_dt, v_bdt), (a_log, v_alog), (d_skip, v_dskip))
    for i, (s, d) in enumerate(small):
        load(("small", i), s, d, small_sem.at[i + 1])
    load(("conv0", 0), conv_in.at[0, 0], conv0.at[0], conv_sem.at[0])
    load(("conv", 0), conv_in.at[0, pl.ds(1, 2)], conv_out.at[0, pl.ds(0, 2)], conv_sem.at[1])
    load(("ssm", 0), ssm_in.at[0], ssm.at[0], ssm_sem.at[0])
    load(("wout", 0), w_out.at[0], v_wout.at[0], wout_sem.at[0])
    for kb in range(KB):
        load(("win", 1, kb), w_in.at[1, pl.ds(kb * KD, KD)], w_raw.at[1, pl.ds(kb * KD, KD)], win_sem.at[1, kb])
    load(("conv0", 1), conv_in.at[1, 0], conv0.at[1], conv_sem.at[2])
    load(("conv", 1), conv_in.at[1, pl.ds(1, 2)], conv_out.at[1, pl.ds(0, 2)], conv_sem.at[3])
    load(("ssm", 1), ssm_in.at[1], ssm.at[1], ssm_sem.at[1])
    load(("wout", 1), w_out.at[1], v_wout.at[1], wout_sem.at[1])

    def make_hidden(l):
        nw = v_norm[...].astype(F32)[l:l + 1, :]

        def step(i, c):
            rows = pl.ds(pl.multiple_of(i * CR, CR), CR)
            hid[rows, :] = (rms(resid[rows, :], 1, 1e-5) * nw).astype(BF16)
            return c

        lax.fori_loop(0, NCH, step, 0)

    def split_weights(l):
        for kb in range(KB):
            copies["win", l, kb].wait()

        def step(kb, c):
            rows = pl.ds(pl.multiple_of(kb * KD, KD), KD)
            for j in range(4):
                s32[j] = w_raw[l, rows, :, j * 128:(j + 1) * 128].reshape(2 * KD, 128).astype(F32)
            for w in range(2):
                for j in range(4):
                    w_xz[w, rows, j * 128:(j + 1) * 128] = s32[j, pl.ds(w, KD, stride=2), :].astype(BF16)
            return c

        lax.fori_loop(0, KB, step, 0)

    def front(l):
        x_b = jnp.dot(hid[...], w_xz[0], preferred_element_type=F32).astype(BF16)
        conv_out[l, 2] = x_b
        gate[...] = silu(jnp.dot(hid[...], w_xz[1], preferred_element_type=F32).astype(BF16).astype(F32))
        copies["conv0", l].wait()
        copies["conv", l].wait()
        cw = v_convw[l].astype(F32)
        pre = v_convb[...].astype(F32)[l:l + 1, :] + cw[3:4, :] * conv_out[l, 2].astype(F32)
        pre = pre + cw[0:1, :] * conv0[l].astype(F32)
        pre = pre + cw[1:2, :] * conv_out[l, 0].astype(F32)
        pre = pre + cw[2:3, :] * conv_out[l, 1].astype(F32)
        xcb[...] = silu(pre).astype(BF16)
        dsx[...] = v_dskip[...][l:l + 1, :] * xcb[...].astype(F32)
        pt = lax.dot_general(v_wxt[l], xcb[...], (((1,), (1,)), ((), ())), preferred_element_type=F32)
        p_half[0] = pt[:, :128]
        p_half[1] = pt[:, 128:]

    def p_sum(l, between):
        p_sa[...] = p_half[1 - core].astype(BF16)
        ca = remote(p_sa, p_ra.at[l], pa_send.at[l], pa_recv.at[l], partner)
        ca.start()
        ca.wait()
        p_sb[...] = (p_half[core] + p_ra[l].astype(F32)).astype(BF16)
        cb = []
        for k in range(1, 4):
            cb.append(remote(p_sb, p_rb.at[l, k - 1], pb_send.at[l, k - 1], pb_recv.at[l, k - 1], lax.rem(me + 2 * k, 8)))
            cb[-1].start()
        between()
        for c in cb:
            c.wait()
        total = jnp.zeros((PW, 128), F32)
        mine = p_sb[...].astype(F32)
        got = [p_rb[l, k].astype(F32) for k in range(3)]
        for chip in range(4):
            d = lax.rem(z - chip + 4, 4)
            term = jnp.where(d == 0, mine, jnp.where(d == 1, got[0], jnp.where(d == 2, got[1], got[2])))
            total = total + term
        p_full[l, core] = total
        cf = remote(p_full.at[l, core], p_full.at[l, core], pf_send.at[l], pf_recv.at[l], partner)
        cf.start()
        cf.wait()

    def steps(l):
        a2[...] = -jnp.exp(v_alog[l]) * LOG2E
        for h in range(2):
            rows = pl.ds(h * 128, 128)
            pt = p_full[l, h]
            low = rms(pt[:RANK].T, 1, 1e-6).astype(BF16)
            lin = jnp.dot(low, v_wdt[l], preferred_element_type=F32) + v_bdt[...][l:l + 1, :]
            dt = jnp.maximum(lin, 0.0) + jnp.log1p(jnp.exp(-jnp.abs(lin)))
            dtb[rows, :] = dt
            dtx[rows, :] = dt * xcb[rows, :].astype(F32)
            b = rms(pt[RANK:RANK + N], 0, 1e-6)
            c = rms(pt[RANK + N:], 0, 1e-6)
            bc = jnp.concatenate([b, c, jnp.zeros((128 - 2 * N, 128), F32)], axis=0)
            bcb[rows, :] = bc.T

    def stage_a(l, i):
        lane = lax.broadcasted_iota(jnp.int32, (1, N, 128), 2)
        sub = lax.broadcasted_iota(jnp.int32, (1, N, 128), 1)
        pick_b = lane == sub
        pick_c = lane == sub + N
        r0 = pl.multiple_of(i * CR, CR)

        def rows8(g, c):
            b0 = pl.multiple_of(r0 + g * 8, 8)
            bc = jnp.broadcast_to(bcb[pl.ds(b0, 8), :][:, None, :], (8, N, 128))
            bcol = jnp.sum(jnp.where(pick_b, bc, 0.0), axis=2, keepdims=True)
            ccol = jnp.sum(jnp.where(pick_c, bc, 0.0), axis=2, keepdims=True)
            for j in range(4):
                cols = pl.ds(j * 128, 128)
                dt8 = dtb[pl.ds(b0, 8), cols]
                dx8 = dtx[pl.ds(b0, 8), cols]
                decay = jnp.exp2(dt8[:, None, :] * a2[:, cols][None])
                new = decay * ssm[l, pl.ds(b0, 8), :, cols] + dx8[:, None, :] * bcol
                ssm[l, pl.ds(b0, 8), :, cols] = new
                y = jnp.sum(new * ccol, axis=1) + dsx[pl.ds(b0, 8), cols]
                gate[pl.ds(b0, 8), cols] = y * gate[pl.ds(b0, 8), cols]
            return c

        lax.fori_loop(0, CR // 8, rows8, 0)
        yg = gate[pl.ds(r0, CR), :].astype(BF16)
        theirs = pl.ds(pl.multiple_of((1 - core) * HALF, HALF), HALF)
        ours = pl.ds(pl.multiple_of(core * HALF, HALF), HALF)
        o_sa[i] = jnp.dot(yg, v_wout[l, :, theirs], preferred_element_type=F32).astype(BF16)
        copy_a(l, i).start()
        own[i] = jnp.dot(yg, v_wout[l, :, ours], preferred_element_type=F32)

    def copy_a(l, i):
        return remote(o_sa.at[i], o_ra.at[l, i], a_send.at[i], a_recv.at[i], partner)

    def copy_b(l, i):
        return remote(o_sb.at[i], o_rb.at[l, i], b_send.at[i], b_recv.at[i], zpair)

    def copy_c(l, i):
        return remote(o_sc.at[i], o_rc.at[l, i], c_send.at[i], c_recv.at[i], midpeer)

    def copy_t(l, i):
        return remote(tot.at[l, core, i], tot.at[l, core, i], t_send.at[i], t_recv.at[i], zpair)

    def copy_f(l, i):
        return remote(tot.at[l, core, i], tot.at[l, core, i], f_send.at[i], f_recv.at[i], partner)

    def stage_b(l, i):
        copy_a(l, i).wait()
        chip = own[i] + o_ra[l, i].astype(F32)

        @pl.when(is_end)
        def _():
            o_sb[i] = chip.astype(BF16)
            copy_b(l, i).start()

        @pl.when(is_mid)
        def _():
            own[i] = chip

    def stage_c(l, i):
        @pl.when(is_mid)
        def _():
            copy_b(l, i).wait_recv()
            o_sc[i] = (own[i] + o_rb[l, i].astype(F32)).astype(BF16)
            copy_c(l, i).start()

        @pl.when(is_end)
        def _():
            copy_b(l, i).wait_send()

    def stage_d(l, i):
        @pl.when(is_mid)
        def _():
            copy_c(l, i).wait()
            tot[l, core, i] = (o_sc[i].astype(F32) + o_rc[l, i].astype(F32)).astype(BF16)
            copy_t(l, i).start()
            copy_f(l, i).start()

    def stage_e(l, i):
        @pl.when(is_end)
        def _():
            copy_t(l, i).wait_recv()
            copy_f(l, i).start()

        @pl.when(is_mid)
        def _():
            copy_t(l, i).wait_send()

    def stage_f(l, i):
        copy_f(l, i).wait()
        rows = pl.ds(pl.multiple_of(i * CR, CR), CR)
        resid[rows, :HALF] = resid[rows, :HALF] + tot[l, 0, i].astype(F32)
        resid[rows, HALF:] = resid[rows, HALF:] + tot[l, 1, i].astype(F32)

    def back(l):
        copies["ssm", l].wait()
        copies["wout", l].wait()

        def step(t, c):
            for off, stage in ((0, stage_a), (OFF_B, stage_b), (OFF_C, stage_c), (OFF_D, stage_d), (OFF_E, stage_e), (OFF_F, stage_f)):
                @pl.when((t >= off) & (t < off + NCH))
                def _():
                    stage(l, t - off)
            return c

        lax.fori_loop(0, NCH + OFF_F, step, 0)

    copies["norm"].wait()
    copies["resid"].wait()
    make_hidden(0)
    split_weights(0)
    for i in range(len(small)):
        copies["small", i].wait()
    front(0)
    pl.semaphore_wait(barrier, 4)
    p_sum(0, lambda: split_weights(1))
    steps(0)
    back(0)
    make_hidden(1)
    front(1)
    p_sum(1, lambda: None)
    steps(1)
    back(1)


def solution(mesh):
    hbm = pl.BlockSpec(memory_space=pl.ANY)
    vmem = pl.BlockSpec(memory_space=pltpu.VMEM)
    V = pltpu.VMEM
    dma = pltpu.SemaphoreType.DMA

    def device_step(residual, norm_w, w_in, conv_w, conv_b, w_x, w_dt, b_dt, a_log, d_skip, w_out, conv_state, ssm_state):
        conv_t = jnp.transpose(conv_state, (0, 2, 1, 3))
        w_xt = jnp.transpose(w_x, (0, 2, 1))
        scratch = [
            V((2, D), BF16), V((2, 4, E), BF16), V((2, E), BF16), V((2, PW, E), BF16), V((2, RANK, E), BF16),
            V((2, E), F32), V((2, N, E), F32), V((2, E), F32),
            V((2, D, 2, E), BF16), V((2, D, E), BF16), V((4, 2 * KD, 128), F32), V((2, E, D), BF16), V((2, ROWS, E), BF16),
            V((ROWS, D), BF16), V((ROWS, E), BF16), V((ROWS, E), F32), V((ROWS, E), F32), V((ROWS, E), F32), V((ROWS, E), F32),
            V((ROWS, 128), F32), V((N, E), F32),
            V((2, PW, 128), F32), V((PW, 128), BF16), V((2, PW, 128), BF16), V((PW, 128), BF16), V((2, 3, PW, 128), BF16),
            V((2, 2, PW, 128), F32),
            V((NCH, CR, HALF), F32), V((NCH, CR, HALF), BF16), V((2, NCH, CR, HALF), BF16), V((NCH, CR, HALF), BF16),
            V((2, NCH, CR, HALF), BF16), V((NCH, CR, HALF), BF16), V((2, NCH, CR, HALF), BF16), V((2, 2, NCH, CR, HALF), BF16),
            dma((8,)), dma, dma((2, KB)), dma((4,)), dma((2,)), dma((2,)),
            dma((2,)), dma((2,)), dma((2, 3)), dma((2, 3)), dma((2,)), dma((2,)),
        ] + [dma((NCH,))] * 10
        resid, conv_out, ssm = pl.pallas_call(
            body,
            out_shape=(V((ROWS, D), F32), V((2, 3, ROWS, E), BF16), V((2, ROWS, N, E), F32)),
            in_specs=[hbm] * 13,
            out_specs=(vmem, vmem, vmem),
            scratch_shapes=scratch,
            compiler_params=pltpu.CompilerParams(collective_id=0, has_side_effects=True, vmem_limit_bytes=42 * 1024 * 1024),
        )(residual, norm_w, w_in, conv_w, conv_b, w_xt, w_dt, b_dt, a_log, d_skip, w_out, conv_t, ssm_state)
        return resid, jnp.transpose(conv_out, (0, 2, 1, 3)), ssm

    cache_spec = P(None, 'dp', None, 'tp')
    in_specs = (P('dp', None), P(None, None), P(None, None, None, 'tp'), P(None, None, 'tp'), P(None, 'tp'), P(None, 'tp', None), P(None, None, 'tp'), P(None, 'tp'), P(None, None, 'tp'), P(None, 'tp'), P(None, 'tp', None), cache_spec, cache_spec)
    out_specs = (P('dp', None), cache_spec, cache_spec)
    return jax.shard_map(device_step, mesh=mesh, in_specs=in_specs, out_specs=out_specs, check_vma=False)
```

```python
import functools

import jax
import jax.numpy as jnp
from jax import lax
from jax.experimental import pallas as pl
from jax.experimental.pallas import tpu as pltpu
from jax.sharding import PartitionSpec as P

MESH = pl.DeviceIdType.MESH
LOG2E = 1.4426950408889634
F32, BF16 = jnp.float32, jnp.bfloat16

ROWS = 256
D = 2048
E = 512
N = 16
RANK = 128
PW = RANK + 2 * N
NCH = 8
CR = ROWS // NCH
HALF = D // 2
KB = 8
KD = D // KB
HR = ROWS // 2
HC = NCH // 2
PH = PW // 2
SPLIT_EARLY = 6
OFF_B, OFF_C, OFF_D, OFF_E, OFF_F = 1, 3, 5, 7, 8
T_FRONT = HC - 1 + OFF_F
P_WAIT = 4
NEXT = T_FRONT + P_WAIT + 1


def silu(v):
    return v * jax.nn.sigmoid(v)


def rms(v, axis, eps):
    return v * lax.rsqrt(jnp.mean(v * v, axis=axis, keepdims=True) + eps)


def body(
    resid_in, norm_w, w_in, conv_w, conv_b, w_xt, w_dt, b_dt, a_log, d_skip, w_out, conv_in, ssm_in,
    resid, conv_out, ssm,
    v_norm, v_convw, v_convb, v_wxt, v_wdt, v_bdt, v_alog, v_dskip,
    w_raw, w_xz, s32, v_wout, conv0,
    hid, xcb, gate, dtb, dtx, dsx, bcb, a2,
    p_own, p_sa, p_ra, p_sb, p_rb, p_full,
    own, o_sa, o_ra, o_sb, o_rb, o_sc, o_rc, tot,
    small_sem, resid_sem, win_sem, conv_sem, ssm_sem, wout_sem,
    pa_send, pa_recv, pb_send, pb_recv, pf_send, pf_recv,
    a_send, a_recv, b_send, b_recv, c_send, c_recv, t_send, t_recv, f_send, f_recv,
):
    dp = lax.axis_index("dp")
    me = lax.axis_index("tp")
    core = lax.rem(me, 2)
    z = me // 2
    is_end = (z == 0) | (z == 3)
    is_mid = (z == 1) | (z == 2)
    partner = me + 1 - 2 * core
    zodd = lax.rem(z, 2)
    zpair = me + 2 - 4 * zodd
    midpeer = (3 - z) * 2 + core

    def dev(t):
        return (dp, t)

    def remote(src, dst, ssem, rsem, target):
        return pltpu.make_async_remote_copy(
            src_ref=src, dst_ref=dst, send_sem=ssem, recv_sem=rsem, device_id=dev(target), device_id_type=MESH)

    barrier = pltpu.get_barrier_semaphore()
    pl.semaphore_signal(barrier, inc=1, device_id=dev(partner), device_id_type=MESH)
    for k in range(1, 4):
        pl.semaphore_signal(barrier, inc=1, device_id=dev(lax.rem(me + 2 * k, 8)), device_id_type=MESH)

    copies = {}

    def load(key, src, dst, sem):
        c = pltpu.make_async_copy(src, dst, sem)
        c.start()
        copies[key] = c

    def wait(key):
        copies.pop(key).wait()

    def load_win(l):
        for kb in range(KB):
            load(("win", l, kb), w_in.at[l, pl.ds(kb * KD, KD)], w_raw.at[l, pl.ds(kb * KD, KD)], win_sem.at[l, kb])

    def load_conv(l):
        load(("conv0", l), conv_in.at[l, 0], conv0.at[l], conv_sem.at[2 * l])
        load(("conv", l), conv_in.at[l, pl.ds(1, 2)], conv_out.at[l, pl.ds(0, 2)], conv_sem.at[2 * l + 1])

    def load_state(l):
        load(("wout", l), w_out.at[l], v_wout.at[l], wout_sem.at[l])
        load(("ssm", l), ssm_in.at[l], ssm.at[l], ssm_sem.at[l])

    load("norm", norm_w, v_norm, small_sem.at[0])
    load("resid", resid_in, resid, resid_sem)
    load_win(0)
    small = ((conv_w, v_convw), (conv_b, v_convb), (w_xt, v_wxt), (w_dt, v_wdt), (b_dt, v_bdt), (a_log, v_alog), (d_skip, v_dskip))
    for i, (s, d) in enumerate(small):
        load(("small", i), s, d, small_sem.at[i + 1])
    load_conv(0)

    def row_of(ref, l):
        v = ref[...].astype(F32)
        return jnp.where(l == 0, v[0:1, :], v[1:2, :])

    def split_block(l, kb):
        rows = pl.ds(pl.multiple_of(kb * KD, KD), KD)
        for j in range(4):
            s32[j] = w_raw[l, rows, :, j * 128:(j + 1) * 128].reshape(2 * KD, 128).astype(F32)
        for w in range(2):
            for j in range(4):
                w_xz[w, rows, j * 128:(j + 1) * 128] = s32[j, pl.ds(w, KD, stride=2), :].astype(BF16)

    def split_blocks(l, lo, hi):
        def step(kb, c):
            split_block(l, kb)
            return c

        lax.fori_loop(lo, hi, step, 0)

    def hidden(l, h):
        nw = row_of(v_norm, l)

        def step(i, c):
            rows = pl.ds(pl.multiple_of(h * HR + i * CR, CR), CR)
            hid[rows, :] = (rms(resid[rows, :], 1, 1e-5) * nw).astype(BF16)
            return c

        lax.fori_loop(0, HR // CR, step, 0)

    def front(l, h):
        rows = pl.ds(pl.multiple_of(h * HR, HR), HR)
        x_b = jnp.dot(hid[rows, :], w_xz[0], preferred_element_type=F32).astype(BF16)
        conv_out[l, 2, rows, :] = x_b
        gate[rows, :] = silu(jnp.dot(hid[rows, :], w_xz[1], preferred_element_type=F32).astype(BF16).astype(F32))
        cw = v_convw[l].astype(F32)
        pre = row_of(v_convb, l) + cw[3:4, :] * conv_out[l, 2, rows, :].astype(F32)
        pre = pre + cw[0:1, :] * conv0[l, rows, :].astype(F32)
        pre = pre + cw[1:2, :] * conv_out[l, 0, rows, :].astype(F32)
        pre = pre + cw[2:3, :] * conv_out[l, 1, rows, :].astype(F32)
        xcb[rows, :] = silu(pre).astype(BF16)
        dsx[rows, :] = row_of(v_dskip, l) * xcb[rows, :].astype(F32)
        p_own[h] = lax.dot_general(v_wxt[l], xcb[rows, :], (((1,), (1,)), ((), ())), preferred_element_type=F32)

    mine = pl.ds(pl.multiple_of(core * PH, PH), PH)
    theirs = pl.ds(pl.multiple_of((1 - core) * PH, PH), PH)

    def copy_pa(l, h):
        return remote(p_sa.at[h], p_ra.at[l, h], pa_send.at[l, h], pa_recv.at[l, h], partner)

    def copy_pb(l, h, k):
        return remote(p_sb.at[h], p_rb.at[l, h, k - 1], pb_send.at[l, h, k - 1], pb_recv.at[l, h, k - 1], lax.rem(me + 2 * k, 8))

    def copy_pf(l, h):
        return remote(p_full.at[l, h, mine], p_full.at[l, h, mine], pf_send.at[l, h], pf_recv.at[l, h], partner)

    def p_one(l, h):
        p_sa[h] = p_own[h, theirs, :].astype(BF16)
        copy_pa(l, h).start()

    def p_two(l, h):
        copy_pa(l, h).wait()
        p_sb[h] = (p_own[h, mine, :] + p_ra[l, h].astype(F32)).astype(BF16)
        for k in range(1, 4):
            copy_pb(l, h, k).start()

    def p_three(l, h):
        for k in range(1, 4):
            copy_pb(l, h, k).wait()
        total = jnp.zeros((PH, HR), F32)
        parts = [p_sb[h].astype(F32)] + [p_rb[l, h, k].astype(F32) for k in range(3)]
        for chip in range(4):
            d = lax.rem(z - chip + 4, 4)
            total = total + jnp.where(d == 0, parts[0], jnp.where(d == 1, parts[1], jnp.where(d == 2, parts[2], parts[3])))
        p_full[l, h, mine, :] = total
        copy_pf(l, h).start()

    def p_four(l, h):
        copy_pf(l, h).wait()
        a2[...] = -jnp.exp(v_alog[l]) * LOG2E
        rows = pl.ds(pl.multiple_of(h * HR, HR), HR)
        pt = p_full[l, h]
        low = rms(pt[:RANK].T, 1, 1e-6).astype(BF16)
        lin = jnp.dot(low, v_wdt[l], preferred_element_type=F32) + row_of(v_bdt, l)
        dt = jnp.maximum(lin, 0.0) + jnp.log1p(jnp.exp(-jnp.abs(lin)))
        dtb[rows, :] = dt
        dtx[rows, :] = dt * xcb[rows, :].astype(F32)
        b = rms(pt[RANK:RANK + N], 0, 1e-6)
        c = rms(pt[RANK + N:], 0, 1e-6)
        bc = jnp.concatenate([b, c, jnp.zeros((128 - 2 * N, HR), F32)], axis=0)
        bcb[rows, :] = bc.T

    def stage_a(l, i):
        lane = lax.broadcasted_iota(jnp.int32, (1, N, 128), 2)
        sub = lax.broadcasted_iota(jnp.int32, (1, N, 128), 1)
        pick_b = lane == sub
        pick_c = lane == sub + N
        r0 = pl.multiple_of(i * CR, CR)

        def rows8(g, c):
            b0 = pl.multiple_of(r0 + g * 8, 8)
            bc = jnp.broadcast_to(bcb[pl.ds(b0, 8), :][:, None, :], (8, N, 128))
            bcol = jnp.sum(jnp.where(pick_b, bc, 0.0), axis=2, keepdims=True)
            ccol = jnp.sum(jnp.where(pick_c, bc, 0.0), axis=2, keepdims=True)
            for j in range(4):
                cols = pl.ds(j * 128, 128)
                dt8 = dtb[pl.ds(b0, 8), cols]
                dx8 = dtx[pl.ds(b0, 8), cols]
                decay = jnp.exp2(dt8[:, None, :] * a2[:, cols][None])
                new = decay * ssm[l, pl.ds(b0, 8), :, cols] + dx8[:, None, :] * bcol
                ssm[l, pl.ds(b0, 8), :, cols] = new
                y = jnp.sum(new * ccol, axis=1) + dsx[pl.ds(b0, 8), cols]
                gate[pl.ds(b0, 8), cols] = y * gate[pl.ds(b0, 8), cols]
            return c

        lax.fori_loop(0, CR // 8, rows8, 0)
        yg = gate[pl.ds(r0, CR), :].astype(BF16)
        their_cols = pl.ds(pl.multiple_of((1 - core) * HALF, HALF), HALF)
        our_cols = pl.ds(pl.multiple_of(core * HALF, HALF), HALF)
        o_sa[i] = jnp.dot(yg, v_wout[l, :, their_cols], preferred_element_type=F32).astype(BF16)
        copy_a(l, i).start()
        own[i] = jnp.dot(yg, v_wout[l, :, our_cols], preferred_element_type=F32)

    def copy_a(l, i):
        return remote(o_sa.at[i], o_ra.at[l, i], a_send.at[l, i], a_recv.at[l, i], partner)

    def copy_b(l, i):
        return remote(o_sb.at[i], o_rb.at[l, i], b_send.at[l, i], b_recv.at[l, i], zpair)

    def copy_c(l, i):
        return remote(o_sc.at[i], o_rc.at[l, i], c_send.at[l, i], c_recv.at[l, i], midpeer)

    def copy_t(l, i):
        return remote(tot.at[l, core, i], tot.at[l, core, i], t_send.at[l, i], t_recv.at[l, i], zpair)

    def copy_f(l, i):
        return remote(tot.at[l, core, i], tot.at[l, core, i], f_send.at[l, i], f_recv.at[l, i], partner)

    def stage_b(l, i):
        copy_a(l, i).wait()
        chip = own[i] + o_ra[l, i].astype(F32)

        @pl.when(is_end)
        def _():
            o_sb[i] = chip.astype(BF16)
            copy_b(l, i).start()

        @pl.when(is_mid)
        def _():
            own[i] = chip

    def stage_c(l, i):
        @pl.when(is_mid)
        def _():
            copy_b(l, i).wait_recv()
            o_sc[i] = (own[i] + o_rb[l, i].astype(F32)).astype(BF16)
            copy_c(l, i).start()

        @pl.when(is_end)
        def _():
            copy_b(l, i).wait_send()

    def stage_d(l, i):
        @pl.when(is_mid)
        def _():
            copy_c(l, i).wait()
            tot[l, core, i] = (o_sc[i].astype(F32) + o_rc[l, i].astype(F32)).astype(BF16)
            copy_t(l, i).start()
            copy_f(l, i).start()

    def stage_e(l, i):
        @pl.when(is_end)
        def _():
            copy_t(l, i).wait_recv()
            copy_f(l, i).start()

        @pl.when(is_mid)
        def _():
            copy_t(l, i).wait_send()

    def stage_f(l, i):
        copy_f(l, i).wait()
        rows = pl.ds(pl.multiple_of(i * CR, CR), CR)
        resid[rows, :HALF] = resid[rows, :HALF] + tot[l, 0, i].astype(F32)
        resid[rows, HALF:] = resid[rows, HALF:] + tot[l, 1, i].astype(F32)

    wait("norm")
    wait("resid")
    hidden(0, 0)
    hidden(0, 1)
    for kb in range(KB):
        wait(("win", 0, kb))
    split_blocks(0, 0, KB)
    load_win(1)
    load_state(0)
    load_conv(1)
    load_state(1)
    for i in range(len(small)):
        wait(("small", i))
    wait(("conv0", 0))
    wait(("conv", 0))

    def first(h, c):
        front(0, h)

        @pl.when(h == 0)
        def _():
            pl.semaphore_wait(barrier, 4)

        p_one(0, h)
        return c

    lax.fori_loop(0, 2, first, 0)
    p_two(0, 0)
    p_two(0, 1)
    for kb in range(KB):
        wait(("win", 1, kb))
    split_blocks(1, 0, SPLIT_EARLY)
    p_three(0, 0)
    p_three(0, 1)
    wait(("wout", 0))
    wait(("ssm", 0))
    wait(("conv0", 1))
    wait(("conv", 1))
    p_four(0, 0)
    p_four(0, 1)
    wait(("wout", 1))
    wait(("ssm", 1))

    def step(t, c):
        def chunks(off, stage):
            v = t - off
            l = jnp.where(v >= NEXT, 1, 0)
            i = v - NEXT * l

            @pl.when((v >= 0) & (i < NCH))
            def _():
                stage(l, i)

        def halves(at, stage):
            h = jnp.where(t >= at + HC, 1, 0)

            @pl.when((t == at) | (t == at + HC))
            def _():
                stage(1, h)

        halves(T_FRONT + 1, p_two)
        halves(T_FRONT + P_WAIT, p_three)
        halves(NEXT, p_four)
        chunks(0, stage_a)

        @pl.when((t >= HC) & (t < HC + KB - SPLIT_EARLY))
        def _():
            split_block(1, t - HC + SPLIT_EARLY)

        chunks(OFF_B, stage_b)
        chunks(OFF_C, stage_c)
        chunks(OFF_D, stage_d)
        chunks(OFF_E, stage_e)
        chunks(OFF_F, stage_f)

        def enter(l, h):
            hidden(l, h)
            front(l, h)
            p_one(l, h)

        halves(T_FRONT, enter)
        return c

    lax.fori_loop(0, NEXT + NCH + OFF_F, step, 0)


def write_out(resid, conv, ssm, resid_out, conv_out, ssm_out, sem):
    copies = [(resid, resid_out), (conv, conv_out)]
    for l in range(2):
        for q in range(4):
            part = pl.ds(q * (ROWS // 4), ROWS // 4)
            copies.append((ssm.at[l, part], ssm_out.at[l, part]))
    copies = [pltpu.make_async_copy(s, d, sem.at[i]) for i, (s, d) in enumerate(copies)]
    for c in copies:
        c.start()
    for c in copies:
        c.wait()


def solution(mesh):
    hbm = pl.BlockSpec(memory_space=pl.ANY)
    vmem = pl.BlockSpec(memory_space=pltpu.VMEM)
    V = pltpu.VMEM
    dma = pltpu.SemaphoreType.DMA

    def device_step(residual, norm_w, w_in, conv_w, conv_b, w_x, w_dt, b_dt, a_log, d_skip, w_out, conv_state, ssm_state):
        conv_t = jnp.transpose(conv_state, (0, 2, 1, 3))
        w_xt = jnp.transpose(w_x, (0, 2, 1))
        scratch = [
            V((2, D), BF16), V((2, 4, E), BF16), V((2, E), BF16), V((2, PW, E), BF16), V((2, RANK, E), BF16),
            V((2, E), F32), V((2, N, E), F32), V((2, E), F32),
            V((2, D, 2, E), BF16), V((2, D, E), BF16), V((4, 2 * KD, 128), F32), V((2, E, D), BF16), V((2, ROWS, E), BF16),
            V((ROWS, D), BF16), V((ROWS, E), BF16), V((ROWS, E), F32), V((ROWS, E), F32), V((ROWS, E), F32), V((ROWS, E), F32),
            V((ROWS, 128), F32), V((N, E), F32),
            V((2, PW, HR), F32), V((2, PH, HR), BF16), V((2, 2, PH, HR), BF16), V((2, PH, HR), BF16), V((2, 2, 3, PH, HR), BF16),
            V((2, 2, PW, HR), F32),
            V((NCH, CR, HALF), F32), V((NCH, CR, HALF), BF16), V((2, NCH, CR, HALF), BF16), V((NCH, CR, HALF), BF16),
            V((2, NCH, CR, HALF), BF16), V((NCH, CR, HALF), BF16), V((2, NCH, CR, HALF), BF16), V((2, 2, NCH, CR, HALF), BF16),
            dma((8,)), dma, dma((2, KB)), dma((4,)), dma((2,)), dma((2,)),
            dma((2, 2)), dma((2, 2)), dma((2, 2, 3)), dma((2, 2, 3)), dma((2, 2)), dma((2, 2)),
        ] + [dma((2, NCH))] * 10
        resid, conv_out, ssm = pl.pallas_call(
            body,
            out_shape=(V((ROWS, D), F32), V((2, 3, ROWS, E), BF16), V((2, ROWS, N, E), F32)),
            in_specs=[hbm] * 13,
            out_specs=(vmem, vmem, vmem),
            scratch_shapes=scratch,
            compiler_params=pltpu.CompilerParams(collective_id=0, has_side_effects=True, vmem_limit_bytes=42 * 1024 * 1024),
        )(residual, norm_w, w_in, conv_w, conv_b, w_xt, w_dt, b_dt, a_log, d_skip, w_out, conv_t, ssm_state)
        resid, conv_out, ssm = (pltpu.with_memory_space_constraint(v, V) for v in (resid, conv_out, ssm))
        resid, conv_out, ssm = pl.pallas_call(
            write_out,
            out_shape=[jax.ShapeDtypeStruct(v.shape, v.dtype) for v in (resid, conv_out, ssm)],
            in_specs=[vmem] * 3,
            out_specs=[hbm] * 3,
            scratch_shapes=[dma((10,))],
            compiler_params=pltpu.CompilerParams(vmem_limit_bytes=24 * 1024 * 1024),
        )(resid, conv_out, ssm)
        return resid, jnp.transpose(conv_out, (0, 2, 1, 3)), ssm

    cache_spec = P(None, 'dp', None, 'tp')
    in_specs = (P('dp', None), P(None, None), P(None, None, None, 'tp'), P(None, None, 'tp'), P(None, 'tp'), P(None, 'tp', None), P(None, None, 'tp'), P(None, 'tp'), P(None, None, 'tp'), P(None, 'tp'), P(None, 'tp', None), cache_spec, cache_spec)
    out_specs = (P('dp', None), cache_spec, cache_spec)
    return jax.shard_map(device_step, mesh=mesh, in_specs=in_specs, out_specs=out_specs, check_vma=False)
```

```python
import functools

import jax
import jax.numpy as jnp
from jax import lax
from jax.experimental import pallas as pl
from jax.experimental.pallas import tpu as pltpu
from jax.sharding import PartitionSpec as P

MESH = pl.DeviceIdType.MESH
LOG2E = 1.4426950408889634
F32, BF16 = jnp.float32, jnp.bfloat16

ROWS = 256
D = 2048
E = 512
N = 16
RANK = 128
PW = RANK + 2 * N
NCH = 8
CR = ROWS // NCH
HALF = D // 2
KB = 8
KD = D // KB
HR = ROWS // 2
HC = NCH // 2
PH = PW // 2
OFF_B, OFF_C, OFF_D, OFF_E, OFF_F, OFF_G = 1, 4, 7, 10, 11, 13
T_FRONT = HC - 1 + OFF_F
P_WAIT = 4
NEXT = T_FRONT + P_WAIT + 1


def silu(v):
    return v * jax.nn.sigmoid(v)


def rms(v, axis, eps):
    return v * lax.rsqrt(jnp.mean(v * v, axis=axis, keepdims=True) + eps)


def body(
    resid_in, norm_w, w_in, conv_w, conv_b, w_xt, w_dt, b_dt, a_log, d_skip, w_out, conv_in, ssm_in,
    resid, conv_out, ssm,
    v_norm, v_convw, v_convb, v_wxt, v_wdt, v_bdt, v_alog, v_dskip,
    w_raw, w_xz, s32, v_wout, conv0,
    hid, xcb, gate, dtb, dtx, dsx, bcb, a2,
    p_own, p_sa, p_ra, p_sb, p_rb, p_full,
    own, o_sa, o_ra, o_sb, o_rb, o_sc, o_rc, tot,
    small_sem, resid_sem, win_sem, conv_sem, ssm_sem, wout_sem,
    pa_send, pa_recv, pb_send, pb_recv, pf_send, pf_recv,
    a_send, a_recv, b_send, b_recv, c_send, c_recv, t_send, t_recv, f_send, f_recv,
):
    dp = lax.axis_index("dp")
    me = lax.axis_index("tp")
    core = lax.rem(me, 2)
    z = me // 2
    is_end = (z == 0) | (z == 3)
    is_mid = (z == 1) | (z == 2)
    partner = me + 1 - 2 * core
    zodd = lax.rem(z, 2)
    zpair = me + 2 - 4 * zodd
    midpeer = (3 - z) * 2 + core

    def dev(t):
        return (dp, t)

    def remote(src, dst, ssem, rsem, target):
        return pltpu.make_async_remote_copy(
            src_ref=src, dst_ref=dst, send_sem=ssem, recv_sem=rsem, device_id=dev(target), device_id_type=MESH)

    barrier = pltpu.get_barrier_semaphore()
    pl.semaphore_signal(barrier, inc=1, device_id=dev(partner), device_id_type=MESH)
    for k in range(1, 4):
        pl.semaphore_signal(barrier, inc=1, device_id=dev(lax.rem(me + 2 * k, 8)), device_id_type=MESH)

    copies = {}

    def load(key, src, dst, sem):
        c = pltpu.make_async_copy(src, dst, sem)
        c.start()
        copies[key] = c

    def wait(key):
        copies.pop(key).wait()

    def load_win(l):
        for kb in range(KB):
            rows = pl.ds(kb * KD, KD)
            for j in range(4):
                pltpu.make_async_copy(w_in.at[l, rows, :, pl.ds(j * 128, 128)], w_raw.at[l, kb, j], win_sem.at[kb]).start()
            copies["win", l, kb] = pltpu.make_async_copy(w_raw.at[l, kb], w_raw.at[l, kb], win_sem.at[kb])

    def load_conv(l):
        load(("conv0", l), conv_in.at[l, 0], conv0.at[l], conv_sem.at[2 * l])
        load(("conv", l), conv_in.at[l, pl.ds(1, 2)], conv_out.at[l, pl.ds(0, 2)], conv_sem.at[2 * l + 1])

    def load_state(l):
        load(("wout", l), w_out.at[l], v_wout.at[l], wout_sem.at[l])
        for n in range(N):
            pltpu.make_async_copy(ssm_in.at[l, :, n, :], ssm.at[l, n], ssm_sem.at[l]).start()
        copies["ssm", l] = pltpu.make_async_copy(ssm.at[l], ssm.at[l], ssm_sem.at[l])

    load("norm", norm_w, v_norm, small_sem.at[0])
    for i in range(NCH):
        load(("resid", i), resid_in.at[pl.ds(i * CR, CR)], resid.at[pl.ds(i * CR, CR)], resid_sem.at[i])
    load_win(0)
    small = ((conv_w, v_convw), (conv_b, v_convb), (w_xt, v_wxt), (w_dt, v_wdt), (b_dt, v_bdt), (a_log, v_alog), (d_skip, v_dskip))
    for i, (s, d) in enumerate(small):
        load(("small", i), s, d, small_sem.at[i + 1])
    load_conv(0)

    late = [("wout", 1), ("conv0", 1), ("conv", 1)] + [("ssm", 1)]

    def row_of(ref, l):
        v = ref[...].astype(F32)
        return jnp.where(l == 0, v[0:1, :], v[1:2, :])

    def unpack(l, kb):
        for j in range(4):
            s32[kb, j] = w_raw[l, kb, j].reshape(2 * KD, 128).astype(F32)

    def pack(kb):
        rows = pl.ds(pl.multiple_of(kb * KD, KD), KD)
        for w in range(2):
            for j in range(4):
                w_xz[w, rows, j * 128:(j + 1) * 128] = s32[kb, j, pl.ds(w, KD, stride=2), :].astype(BF16)

    def normed(l, i):
        rows = pl.ds(pl.multiple_of(i * CR, CR), CR)
        hid[rows, :] = (rms(resid[rows, :], 1, 1e-5) * row_of(v_norm, l)).astype(BF16)

    def hidden(l, h):
        def step(i, c):
            normed(l, h * HC + i)
            return c

        lax.fori_loop(0, HC, step, 0)

    def front(l, h):
        rows = pl.ds(pl.multiple_of(h * HR, HR), HR)
        x_b = jnp.dot(hid[rows, :], w_xz[0], preferred_element_type=F32).astype(BF16)
        conv_out[l, 2, rows, :] = x_b
        gate[rows, :] = silu(jnp.dot(hid[rows, :], w_xz[1], preferred_element_type=F32).astype(BF16).astype(F32))
        cw = v_convw[l].astype(F32)
        pre = row_of(v_convb, l) + cw[3:4, :] * conv_out[l, 2, rows, :].astype(F32)
        pre = pre + cw[0:1, :] * conv0[l, rows, :].astype(F32)
        pre = pre + cw[1:2, :] * conv_out[l, 0, rows, :].astype(F32)
        pre = pre + cw[2:3, :] * conv_out[l, 1, rows, :].astype(F32)
        xcb[rows, :] = silu(pre).astype(BF16)
        dsx[rows, :] = row_of(v_dskip, l) * xcb[rows, :].astype(F32)
        p_own[h] = lax.dot_general(v_wxt[l], xcb[rows, :], (((1,), (1,)), ((), ())), preferred_element_type=F32)

    mine = pl.ds(pl.multiple_of(core * PH, PH), PH)
    theirs = pl.ds(pl.multiple_of((1 - core) * PH, PH), PH)

    def copy_pa(l, h):
        return remote(p_sa.at[l, h], p_ra.at[l, h], pa_send.at[h], pa_recv.at[h], partner)

    def copy_pb(l, h, k):
        return remote(p_sb.at[l, h], p_rb.at[l, h, k - 1], pb_send.at[h, k - 1], pb_recv.at[h, k - 1], lax.rem(me + 2 * k, 8))

    def copy_pf(l, h):
        return remote(p_full.at[l, h, mine], p_full.at[l, h, mine], pf_send.at[h], pf_recv.at[h], partner)

    def p_one(l, h):
        p_sa[l, h] = p_own[h, theirs, :].astype(BF16)
        copy_pa(l, h).start()

    def p_two(l, h):
        copy_pa(l, h).wait_recv()
        p_sb[l, h] = (p_own[h, mine, :] + p_ra[l, h].astype(F32)).astype(BF16)
        for k in range(1, 4):
            copy_pb(l, h, k).start()

    def p_three(l, h):
        for k in range(1, 4):
            copy_pb(l, h, k).wait_recv()
        total = jnp.zeros((PH, HR), F32)
        parts = [p_sb[l, h].astype(F32)] + [p_rb[l, h, k].astype(F32) for k in range(3)]
        for chip in range(4):
            d = lax.rem(z - chip + 4, 4)
            total = total + jnp.where(d == 0, parts[0], jnp.where(d == 1, parts[1], jnp.where(d == 2, parts[2], parts[3])))
        p_full[l, h, mine, :] = total
        copy_pf(l, h).start()

    def p_left(l, h):
        copy_pa(l, h).wait_send()
        for k in range(1, 4):
            copy_pb(l, h, k).wait_send()
        copy_pf(l, h).wait_send()

    def rates(l):
        for n in range(N):
            a2[l, n] = jnp.broadcast_to(-jnp.exp(v_alog[l, n:n + 1, :]) * LOG2E, (8, E))

    def p_four(l, h):
        copy_pf(l, h).wait_recv()
        rows = pl.ds(pl.multiple_of(h * HR, HR), HR)
        pt = p_full[l, h]
        low = rms(pt[:RANK].T, 1, 1e-6).astype(BF16)
        lin = jnp.dot(low, v_wdt[l], preferred_element_type=F32) + row_of(v_bdt, l)
        dt = jnp.maximum(lin, 0.0) + jnp.log1p(jnp.exp(-jnp.abs(lin)))
        dtb[rows, :] = dt
        dtx[rows, :] = dt * xcb[rows, :].astype(F32)
        b = rms(pt[RANK:RANK + N], 0, 1e-6)
        c = rms(pt[RANK + N:], 0, 1e-6)
        bc = jnp.concatenate([b, c, jnp.zeros((128 - 2 * N, HR), F32)], axis=0)
        bcb[rows, :] = bc.T

    def stage_a(l, i):
        r0 = pl.multiple_of(i * CR, CR)

        rows = pl.ds(r0, CR)
        bc = bcb[rows, :]
        dt = dtb[rows, :]
        dx = dtx[rows, :]
        y = dsx[rows, :]
        for n in range(N):
            rate = jnp.concatenate([a2[l, n]] * (CR // 8), axis=0)
            new = jnp.exp2(dt * rate) * ssm[l, n, rows, :] + dx * bc[:, n:n + 1]
            ssm[l, n, rows, :] = new
            y = y + new * bc[:, N + n:N + n + 1]
        yg = (y * gate[rows, :]).astype(BF16)
        their_cols = pl.ds(pl.multiple_of((1 - core) * HALF, HALF), HALF)
        our_cols = pl.ds(pl.multiple_of(core * HALF, HALF), HALF)
        o_sa[i] = jnp.dot(yg, v_wout[l, :, their_cols], preferred_element_type=F32).astype(BF16)
        copy_a(l, i).start()
        own[i] = jnp.dot(yg, v_wout[l, :, our_cols], preferred_element_type=F32)

    def copy_a(l, i):
        return remote(o_sa.at[i], o_ra.at[l, i], a_send.at[i], a_recv.at[i], partner)

    def copy_b(l, i):
        return remote(o_sb.at[i], o_rb.at[l, i], b_send.at[i], b_recv.at[i], zpair)

    def copy_c(l, i):
        return remote(o_sc.at[i], o_rc.at[l, i], c_send.at[i], c_recv.at[i], midpeer)

    def copy_t(l, i):
        return remote(tot.at[l, core, i], tot.at[l, core, i], t_send.at[i], t_recv.at[i], zpair)

    def copy_f(l, i):
        return remote(tot.at[l, core, i], tot.at[l, core, i], f_send.at[i], f_recv.at[i], partner)

    def stage_b(l, i):
        copy_a(l, i).wait_recv()
        chip = own[i] + o_ra[l, i].astype(F32)

        @pl.when(is_end)
        def _():
            o_sb[i] = chip.astype(BF16)
            copy_b(l, i).start()

        @pl.when(is_mid)
        def _():
            own[i] = chip

    def stage_c(l, i):
        @pl.when(is_mid)
        def _():
            copy_b(l, i).wait_recv()
            o_sc[i] = (own[i] + o_rb[l, i].astype(F32)).astype(BF16)
            copy_c(l, i).start()

    def stage_d(l, i):
        @pl.when(is_mid)
        def _():
            copy_c(l, i).wait_recv()
            tot[l, core, i] = (o_sc[i].astype(F32) + o_rc[l, i].astype(F32)).astype(BF16)
            copy_t(l, i).start()
            copy_f(l, i).start()

    def stage_e(l, i):
        @pl.when(is_end)
        def _():
            copy_t(l, i).wait_recv()
            copy_f(l, i).start()

    def stage_f(l, i):
        copy_f(l, i).wait_recv()
        rows = pl.ds(pl.multiple_of(i * CR, CR), CR)
        resid[rows, :HALF] = resid[rows, :HALF] + tot[l, 0, i].astype(F32)
        resid[rows, HALF:] = resid[rows, HALF:] + tot[l, 1, i].astype(F32)

    def stage_g(l, i):
        copy_a(l, i).wait_send()
        copy_f(l, i).wait_send()

        @pl.when(is_end)
        def _():
            copy_b(l, i).wait_send()

        @pl.when(is_mid)
        def _():
            copy_c(l, i).wait_send()
            copy_t(l, i).wait_send()

    wait("norm")
    for i in range(NCH):
        wait(("resid", i))
        normed(0, i)
    for kb in range(KB):
        wait(("win", 0, kb))
        unpack(0, kb)
        if kb > 0:
            pack(kb - 1)
    pack(KB - 1)
    load_win(1)
    load_state(0)
    for i in range(len(small)):
        wait(("small", i))
    wait(("conv0", 0))
    wait(("conv", 0))

    def first(h, c):
        front(0, h)

        @pl.when(h == 0)
        def _():
            pl.semaphore_wait(barrier, 4)

        p_one(0, h)
        return c

    lax.fori_loop(0, 2, first, 0)
    p_two(0, 0)
    rates(0)
    rates(1)
    for kb in range(KB):
        wait(("win", 1, kb))

    def unpack_next(kb, c):
        unpack(1, kb)
        return c

    def pack_next(kb, c):
        pack(kb)
        return c

    lax.fori_loop(0, KB, unpack_next, 0)
    p_two(0, 1)
    lax.fori_loop(0, KB, pack_next, 0)
    p_three(0, 0)
    load_conv(1)
    load_state(1)
    for key in [k for k in copies if k not in late]:
        wait(key)
    p_four(0, 0)

    def arrived():
        for key in late:
            wait(key)

    def step(t, c):
        def chunks(off, stage):
            v = t - off
            l = jnp.where(v >= NEXT, 1, 0)
            i = v - NEXT * l

            @pl.when((v >= 0) & (i < NCH))
            def _():
                stage(l, i)

        def halves(at, stage, first_at=None):
            h = jnp.where(t == at, 0, 1)
            l = jnp.where(t >= at, 1, 0)
            now = (t == at) | (t == at + HC)
            if first_at is not None:
                now = now | (t == first_at)

            @pl.when(now)
            def _():
                stage(l, h)

        def enter(l, h):
            hidden(l, h)
            front(l, h)
            p_one(l, h)

        @pl.when(t == NCH)
        def _():
            arrived()
            for h in range(2):
                p_left(0, h)

        halves(NEXT, p_four, HC)
        chunks(0, stage_a)
        chunks(OFF_B, stage_b)
        chunks(OFF_C, stage_c)
        chunks(OFF_D, stage_d)
        halves(T_FRONT + 1, p_two)
        chunks(OFF_E, stage_e)
        chunks(OFF_F, stage_f)
        halves(T_FRONT, enter)
        halves(T_FRONT + P_WAIT, p_three, 2)
        chunks(OFF_G, stage_g)
        return c

    lax.fori_loop(0, NEXT + NCH + OFF_G, step, 0)
    for h in range(2):
        p_left(1, h)


def write_out(resid, conv, ssm, resid_out, conv_out, ssm_out, sem):
    for l in range(2):
        for n in range(N):
            pltpu.make_async_copy(ssm.at[l, n], ssm_out.at[l, :, n, :], sem.at[0]).start()
    others = [pltpu.make_async_copy(resid, resid_out, sem.at[1]), pltpu.make_async_copy(conv, conv_out, sem.at[2])]
    for c in others:
        c.start()
    for c in others:
        c.wait()
    pltpu.make_async_copy(ssm, ssm, sem.at[0]).wait()


def solution(mesh):
    hbm = pl.BlockSpec(memory_space=pl.ANY)
    vmem = pl.BlockSpec(memory_space=pltpu.VMEM)
    V = pltpu.VMEM
    dma = pltpu.SemaphoreType.DMA

    def device_step(residual, norm_w, w_in, conv_w, conv_b, w_x, w_dt, b_dt, a_log, d_skip, w_out, conv_state, ssm_state):
        conv_t = jnp.transpose(conv_state, (0, 2, 1, 3))
        w_xt = jnp.transpose(w_x, (0, 2, 1))
        scratch = [
            V((2, D), BF16), V((2, 4, E), BF16), V((2, E), BF16), V((2, PW, E), BF16), V((2, RANK, E), BF16),
            V((2, E), F32), V((2, N, E), F32), V((2, E), F32),
            V((2, KB, 4, KD, 2, 128), BF16), V((2, D, E), BF16), V((KB, 4, 2 * KD, 128), F32), V((2, E, D), BF16), V((2, ROWS, E), BF16),
            V((ROWS, D), BF16), V((ROWS, E), BF16), V((ROWS, E), F32), V((ROWS, E), F32), V((ROWS, E), F32), V((ROWS, E), F32),
            V((ROWS, 128), F32), V((2, N, 8, E), F32),
            V((2, PW, HR), F32), V((2, 2, PH, HR), BF16), V((2, 2, PH, HR), BF16), V((2, 2, PH, HR), BF16), V((2, 2, 3, PH, HR), BF16),
            V((2, 2, PW, HR), F32),
            V((NCH, CR, HALF), F32), V((NCH, CR, HALF), BF16), V((2, NCH, CR, HALF), BF16), V((NCH, CR, HALF), BF16),
            V((2, NCH, CR, HALF), BF16), V((NCH, CR, HALF), BF16), V((2, NCH, CR, HALF), BF16), V((2, 2, NCH, CR, HALF), BF16),
            dma((8,)), dma((NCH,)), dma((KB,)), dma((4,)), dma((2,)), dma((2,)),
            dma((2,)), dma((2,)), dma((2, 3)), dma((2, 3)), dma((2,)), dma((2,)),
        ] + [dma((NCH,))] * 10
        resid, conv_out, ssm = pl.pallas_call(
            body,
            out_shape=(V((ROWS, D), F32), V((2, 3, ROWS, E), BF16), V((2, N, ROWS, E), F32)),
            in_specs=[hbm] * 13,
            out_specs=(vmem, vmem, vmem),
            scratch_shapes=scratch,
            compiler_params=pltpu.CompilerParams(collective_id=0, has_side_effects=True, vmem_limit_bytes=43 * 1024 * 1024),
        )(residual, norm_w, w_in, conv_w, conv_b, w_xt, w_dt, b_dt, a_log, d_skip, w_out, conv_t, ssm_state)
        resid, conv_out, ssm = (pltpu.with_memory_space_constraint(v, V) for v in (resid, conv_out, ssm))
        resid, conv_out, ssm = pl.pallas_call(
            write_out,
            out_shape=[jax.ShapeDtypeStruct(v.shape, v.dtype) for v in (resid, conv_out, ssm_state)],
            in_specs=[vmem] * 3,
            out_specs=[hbm] * 3,
            scratch_shapes=[dma((3,))],
            compiler_params=pltpu.CompilerParams(vmem_limit_bytes=24 * 1024 * 1024),
        )(resid, conv_out, ssm)
        return resid, jnp.transpose(conv_out, (0, 2, 1, 3)), ssm

    cache_spec = P(None, 'dp', None, 'tp')
    in_specs = (P('dp', None), P(None, None), P(None, None, None, 'tp'), P(None, None, 'tp'), P(None, 'tp'), P(None, 'tp', None), P(None, None, 'tp'), P(None, 'tp'), P(None, None, 'tp'), P(None, 'tp'), P(None, 'tp', None), cache_spec, cache_spec)
    out_specs = (P('dp', None), cache_spec, cache_spec)
    return jax.shard_map(device_step, mesh=mesh, in_specs=in_specs, out_specs=out_specs, check_vma=False)
```

```python
import functools

import jax
import jax.numpy as jnp
from jax import lax
from jax.experimental import pallas as pl
from jax.experimental.pallas import tpu as pltpu
from jax.sharding import PartitionSpec as P

MESH = pl.DeviceIdType.MESH
LOG2E = 1.4426950408889634
F32, BF16 = jnp.float32, jnp.bfloat16

ROWS = 256
D = 2048
E = 512
N = 16
RANK = 128
PW = RANK + 2 * N
NCH = 8
CR = ROWS // NCH
HALF = D // 2
KB = 8
KD = D // KB
HR = ROWS // 2
HC = NCH // 2
PH = PW // 2
FIRST = 3
OFF_B, OFF_C, OFF_D, OFF_E, OFF_F = 1, 4, 7, 10, 11
T_FRONT = HC - 1 + OFF_F
P_WAIT = 4
NEXT = T_FRONT + P_WAIT + 1


def silu(v):
    return v * jax.nn.sigmoid(v)


def rms(v, axis, eps):
    return v * lax.rsqrt(jnp.mean(v * v, axis=axis, keepdims=True) + eps)


def body(
    resid_in, norm_w, w_in, conv_w, conv_b, w_xt, w_dt, b_dt, a_log, d_skip, w_out, conv_in, ssm_in,
    resid, conv_out, ssm,
    v_norm, v_convw, v_convb, v_wxt, v_wdt, v_bdt, v_alog, v_dskip,
    w_raw, w_xz, s32, v_wout, conv0,
    hid, xcb, gate, dtb, dtx, dsx, bcb, a2,
    p_own, p_sa, p_ra, p_sb, p_rb, p_full,
    own, o_sa, o_ra, o_sb, o_rb, o_sc, o_rc, tot,
    small_sem, resid_sem, win_sem, conv_sem, ssm_sem, wout_sem,
    pa_send, pa_recv, pb_send, pb_recv, pf_send, pf_recv,
    a_send, a_recv, b_send, b_recv, c_send, c_recv, t_send, t_recv, f_send, f_recv,
):
    dp = lax.axis_index("dp")
    me = lax.axis_index("tp")
    core = lax.rem(me, 2)
    z = me // 2
    is_end = (z == 0) | (z == 3)
    is_mid = (z == 1) | (z == 2)
    partner = me + 1 - 2 * core
    zodd = lax.rem(z, 2)
    zpair = me + 2 - 4 * zodd
    midpeer = (3 - z) * 2 + core

    def dev(t):
        return (dp, t)

    def remote(src, dst, ssem, rsem, target):
        return pltpu.make_async_remote_copy(
            src_ref=src, dst_ref=dst, send_sem=ssem, recv_sem=rsem, device_id=dev(target), device_id_type=MESH)

    barrier = pltpu.get_barrier_semaphore()
    pl.semaphore_signal(barrier, inc=1, device_id=dev(partner), device_id_type=MESH)
    for k in range(1, 4):
        pl.semaphore_signal(barrier, inc=1, device_id=dev(lax.rem(me + 2 * k, 8)), device_id_type=MESH)

    copies = {}

    def load(key, src, dst, sem):
        c = pltpu.make_async_copy(src, dst, sem)
        c.start()
        copies[key] = c

    def wait(key):
        copies.pop(key).wait()

    def load_win(l, blocks):
        for kb in blocks:
            rows = pl.ds(kb * 8 * KD, 8 * KD)
            load(("win", l, kb), w_in.at[l, rows], w_raw.at[l, rows], win_sem.at[l, kb])

    def load_conv(l):
        load(("conv0", l), conv_in.at[l, 0], conv0.at[l], conv_sem.at[2 * l])
        load(("conv", l), conv_in.at[l, pl.ds(1, 2)], conv_out.at[l, pl.ds(0, 2)], conv_sem.at[2 * l + 1])

    def load_state(l):
        load(("wout", l), w_out.at[l], v_wout.at[l], wout_sem.at[l])
        for n in range(N):
            load_plane(l, n)

    def load_plane(l, n):
        pltpu.make_async_copy(ssm_in.at[l, :, n, :], ssm.at[l, n], ssm_sem.at[l]).start()

    def wait_planes(l):
        pltpu.make_async_copy(ssm.at[l], ssm.at[l], ssm_sem.at[l]).wait()

    load("norm", norm_w, v_norm, small_sem.at[0])
    load_win(0, range(FIRST))
    for i in range(HC):
        rows = pl.ds(i * 2 * CR, 2 * CR)
        load(("resid", i), resid_in.at[rows], resid.at[rows], resid_sem.at[i])
    load_win(0, range(FIRST, KB))
    small = ((conv_w, v_convw), (conv_b, v_convb), (w_xt, v_wxt), (w_dt, v_wdt), (b_dt, v_bdt), (a_log, v_alog), (d_skip, v_dskip))
    for i, (s, d) in enumerate(small):
        load(("small", i), s, d, small_sem.at[i + 1])
    load_conv(0)

    def row_of(ref, l):
        v = ref[...].astype(F32)
        return jnp.where(l == 0, v[0:1, :], v[1:2, :])

    def unpack(l, kb):
        s32[kb] = w_raw[l, pl.ds(pl.multiple_of(kb * 8 * KD, 8 * KD), 8 * KD), :].astype(F32)

    def pack(kb):
        rows = pl.ds(pl.multiple_of(kb * KD, KD), KD)
        for w in range(2):
            for j in range(4):
                w_xz[w, rows, j * 128:(j + 1) * 128] = s32[kb, pl.ds(2 * j + w, KD, stride=8), :].astype(BF16)

    def normed(l, i):
        rows = pl.ds(pl.multiple_of(i * CR, CR), CR)
        hid[rows, :] = (rms(resid[rows, :], 1, 1e-5) * row_of(v_norm, l)).astype(BF16)

    def front(l, h):
        rows = pl.ds(pl.multiple_of(h * HR, HR), HR)
        x_b = jnp.dot(hid[rows, :], w_xz[0], preferred_element_type=F32).astype(BF16)
        conv_out[l, 2, rows, :] = x_b
        gate[rows, :] = silu(jnp.dot(hid[rows, :], w_xz[1], preferred_element_type=F32).astype(BF16).astype(F32))
        cw = v_convw[l].astype(F32)
        pre = row_of(v_convb, l) + cw[3:4, :] * conv_out[l, 2, rows, :].astype(F32)
        pre = pre + cw[0:1, :] * conv0[l, rows, :].astype(F32)
        pre = pre + cw[1:2, :] * conv_out[l, 0, rows, :].astype(F32)
        pre = pre + cw[2:3, :] * conv_out[l, 1, rows, :].astype(F32)
        xcb[rows, :] = silu(pre).astype(BF16)
        dsx[rows, :] = row_of(v_dskip, l) * xcb[rows, :].astype(F32)
        p_own[h] = lax.dot_general(v_wxt[l], xcb[rows, :], (((1,), (1,)), ((), ())), preferred_element_type=F32)

    mine = pl.ds(pl.multiple_of(core * PH, PH), PH)
    theirs = pl.ds(pl.multiple_of((1 - core) * PH, PH), PH)

    def copy_pa(l, h):
        return remote(p_sa.at[l, h], p_ra.at[l, h], pa_send.at[h], pa_recv.at[h], partner)

    def copy_pb(l, h, k):
        return remote(p_sb.at[l, h], p_rb.at[l, h, k - 1], pb_send.at[h, k - 1], pb_recv.at[h, k - 1], lax.rem(me + 2 * k, 8))

    def copy_pf(l, h):
        return remote(p_full.at[l, h, mine], p_full.at[l, h, mine], pf_send.at[h], pf_recv.at[h], partner)

    def p_one(l, h):
        p_sa[l, h] = p_own[h, theirs, :].astype(BF16)
        copy_pa(l, h).start()

    def p_two(l, h):
        copy_pa(l, h).wait_recv()
        p_sb[l, h] = (p_own[h, mine, :] + p_ra[l, h].astype(F32)).astype(BF16)
        for k in range(1, 4):
            copy_pb(l, h, k).start()

    def p_three(l, h):
        for k in range(1, 4):
            copy_pb(l, h, k).wait_recv()
        total = jnp.zeros((PH, HR), F32)
        parts = [p_sb[l, h].astype(F32)] + [p_rb[l, h, k].astype(F32) for k in range(3)]
        for chip in range(4):
            d = lax.rem(z - chip + 4, 4)
            total = total + jnp.where(d == 0, parts[0], jnp.where(d == 1, parts[1], jnp.where(d == 2, parts[2], parts[3])))
        p_full[l, h, mine, :] = total
        copy_pf(l, h).start()

    def p_left(l, h):
        copy_pa(l, h).wait_send()
        for k in range(1, 4):
            copy_pb(l, h, k).wait_send()
        copy_pf(l, h).wait_send()

    def rates(l):
        for n in range(N):
            a2[l, n] = jnp.broadcast_to(-jnp.exp(v_alog[l, n:n + 1, :]) * LOG2E, (8, E))

    def p_four(l, h):
        copy_pf(l, h).wait_recv()
        rows = pl.ds(pl.multiple_of(h * HR, HR), HR)
        pt = p_full[l, h]
        low = rms(pt[:RANK].T, 1, 1e-6).astype(BF16)
        lin = jnp.dot(low, v_wdt[l], preferred_element_type=F32) + row_of(v_bdt, l)
        dt = jnp.maximum(lin, 0.0) + jnp.log1p(jnp.exp(-jnp.abs(lin)))
        dtb[rows, :] = dt
        dtx[rows, :] = dt * xcb[rows, :].astype(F32)
        b = rms(pt[RANK:RANK + N], 0, 1e-6)
        c = rms(pt[RANK + N:], 0, 1e-6)
        bc = jnp.concatenate([b, c, jnp.zeros((128 - 2 * N, HR), F32)], axis=0)
        bcb[rows, :] = bc.T

    def stage_a(l, i):
        r0 = pl.multiple_of(i * CR, CR)

        rows = pl.ds(r0, CR)
        bc = bcb[rows, :]
        dt = dtb[rows, :]
        dx = dtx[rows, :]
        y = dsx[rows, :]
        for n in range(N):
            rate = jnp.concatenate([a2[l, n]] * (CR // 8), axis=0)
            new = jnp.exp2(dt * rate) * ssm[l, n, rows, :] + dx * bc[:, n:n + 1]
            ssm[l, n, rows, :] = new
            y = y + new * bc[:, N + n:N + n + 1]
        yg = (y * gate[rows, :]).astype(BF16)
        their_cols = pl.ds(pl.multiple_of((1 - core) * HALF, HALF), HALF)
        our_cols = pl.ds(pl.multiple_of(core * HALF, HALF), HALF)
        o_sa[i] = jnp.dot(yg, v_wout[l, :, their_cols], preferred_element_type=F32).astype(BF16)
        copy_a(l, i).start()
        own[i] = jnp.dot(yg, v_wout[l, :, our_cols], preferred_element_type=F32)

    def copy_a(l, i):
        return remote(o_sa.at[i], o_ra.at[l, i], a_send, a_recv.at[i], partner)

    def copy_b(l, i):
        return remote(o_sb.at[i], o_rb.at[l, i], b_send, b_recv.at[i], zpair)

    def copy_c(l, i):
        return remote(o_sc.at[i], o_rc.at[l, i], c_send, c_recv.at[i], midpeer)

    def copy_t(l, i):
        return remote(tot.at[l, core, i], tot.at[l, core, i], t_send, t_recv.at[i], zpair)

    def copy_f(l, i):
        return remote(tot.at[l, core, i], tot.at[l, core, i], f_send, f_recv.at[i], partner)

    def stage_b(l, i):
        copy_a(l, i).wait_recv()
        chip = own[i] + o_ra[l, i].astype(F32)

        @pl.when(is_end)
        def _():
            o_sb[i] = chip.astype(BF16)
            copy_b(l, i).start()

        @pl.when(is_mid)
        def _():
            own[i] = chip

    def stage_c(l, i):
        @pl.when(is_mid)
        def _():
            copy_b(l, i).wait_recv()
            o_sc[i] = (own[i] + o_rb[l, i].astype(F32)).astype(BF16)
            copy_c(l, i).start()

    def stage_d(l, i):
        @pl.when(is_mid)
        def _():
            copy_c(l, i).wait_recv()
            tot[l, core, i] = (o_sc[i].astype(F32) + o_rc[l, i].astype(F32)).astype(BF16)
            copy_t(l, i).start()
            copy_f(l, i).start()

    def stage_e(l, i):
        @pl.when(is_end)
        def _():
            copy_t(l, i).wait_recv()
            copy_f(l, i).start()

    def stage_f(l, i):
        copy_f(l, i).wait_recv()
        rows = pl.ds(pl.multiple_of(i * CR, CR), CR)
        resid[rows, :HALF] = resid[rows, :HALF] + tot[l, 0, i].astype(F32)
        resid[rows, HALF:] = resid[rows, HALF:] + tot[l, 1, i].astype(F32)

        @pl.when(l == 0)
        def _():
            normed(1, i)

    def o_left(l):
        remote(o_sa, o_sa, a_send, a_recv.at[0], partner).wait_send()
        remote(tot.at[l, core], tot.at[l, core], f_send, f_recv.at[0], partner).wait_send()

        @pl.when(is_end)
        def _():
            remote(o_sb, o_sb, b_send, b_recv.at[0], zpair).wait_send()

        @pl.when(is_mid)
        def _():
            remote(o_sc, o_sc, c_send, c_recv.at[0], midpeer).wait_send()
            remote(tot.at[l, core], tot.at[l, core], t_send, t_recv.at[0], zpair).wait_send()

    for kb in range(KB):
        if kb == FIRST:
            wait("norm")
            for i in range(HC):
                wait(("resid", i))
                normed(0, 2 * i)
                normed(0, 2 * i + 1)
            load_state(0)
            load_win(1, range(KB))
        wait(("win", 0, kb))
        unpack(0, kb)
        if kb > 0:
            pack(kb - 1)
    pack(KB - 1)
    for i in range(len(small)):
        wait(("small", i))
    wait(("conv0", 0))
    wait(("conv", 0))

    def first(h, c):
        front(0, h)

        @pl.when(h == 0)
        def _():
            pl.semaphore_wait(barrier, 4)

        p_one(0, h)
        return c

    lax.fori_loop(0, 2, first, 0)
    p_two(0, 0)
    rates(0)
    rates(1)
    for kb in range(KB):
        wait(("win", 1, kb))

    def unpack_next(kb, c):
        unpack(1, kb)
        return c

    def pack_next(kb, c):
        pack(kb)
        return c

    lax.fori_loop(0, KB, unpack_next, 0)
    p_two(0, 1)
    lax.fori_loop(0, KB, pack_next, 0)
    p_three(0, 0)
    wait(("wout", 0))
    wait_planes(0)
    load_conv(1)
    load(("wout", 1), w_out.at[1], v_wout.at[1], wout_sem.at[1])
    p_four(0, 0)

    def step(t, c):
        def chunks(off, stage):
            v = t - off
            l = jnp.where(v >= NEXT, 1, 0)
            i = v - NEXT * l

            @pl.when((v >= 0) & (i < NCH))
            def _():
                stage(l, i)

        def halves(at, stage, first_at=None):
            h = jnp.where(t == at, 0, 1)
            l = jnp.where(t >= at, 1, 0)
            now = (t == at) | (t == at + HC)
            if first_at is not None:
                now = now | (t == first_at)

            @pl.when(now)
            def _():
                stage(l, h)

        def enter(l, h):
            front(l, h)
            p_one(l, h)

        @pl.when(t < N)
        def _():
            load_plane(1, t)

        @pl.when(t == T_FRONT)
        def _():
            for h in range(2):
                p_left(0, h)
            for key in (("wout", 1), ("conv0", 1), ("conv", 1)):
                wait(key)

        @pl.when(t == NEXT)
        def _():
            wait_planes(1)
            o_left(0)

        halves(NEXT, p_four, HC)
        chunks(0, stage_a)
        chunks(OFF_B, stage_b)
        chunks(OFF_C, stage_c)
        chunks(OFF_D, stage_d)
        halves(T_FRONT + 1, p_two)
        chunks(OFF_E, stage_e)
        chunks(OFF_F, stage_f)
        halves(T_FRONT, enter)
        halves(T_FRONT + P_WAIT, p_three, 2)
        return c

    lax.fori_loop(0, NEXT + NCH + OFF_F, step, 0)
    o_left(1)
    for h in range(2):
        p_left(1, h)


def write_out(resid, conv, ssm, resid_out, conv_out, ssm_out, sem):
    for l in range(2):
        for n in range(N):
            pltpu.make_async_copy(ssm.at[l, n], ssm_out.at[l, :, n, :], sem.at[0]).start()
    others = [pltpu.make_async_copy(resid, resid_out, sem.at[1]), pltpu.make_async_copy(conv, conv_out, sem.at[2])]
    for c in others:
        c.start()
    for c in others:
        c.wait()
    pltpu.make_async_copy(ssm, ssm, sem.at[0]).wait()


def solution(mesh):
    hbm = pl.BlockSpec(memory_space=pl.ANY)
    vmem = pl.BlockSpec(memory_space=pltpu.VMEM)
    V = pltpu.VMEM
    dma = pltpu.SemaphoreType.DMA

    def device_step(residual, norm_w, w_in, conv_w, conv_b, w_x, w_dt, b_dt, a_log, d_skip, w_out, conv_state, ssm_state):
        conv_t = jnp.transpose(conv_state, (0, 2, 1, 3))
        w_xt = jnp.transpose(w_x, (0, 2, 1))
        w_rows = jnp.transpose(w_in.reshape(2, D, 2, 4, 128), (0, 1, 3, 2, 4)).reshape(2, 8 * D, 128)
        scratch = [
            V((2, D), BF16), V((2, 4, E), BF16), V((2, E), BF16), V((2, PW, E), BF16), V((2, RANK, E), BF16),
            V((2, E), F32), V((2, N, E), F32), V((2, E), F32),
            V((2, 8 * D, 128), BF16), V((2, D, E), BF16), V((KB, 8 * KD, 128), F32), V((2, E, D), BF16), V((2, ROWS, E), BF16),
            V((ROWS, D), BF16), V((ROWS, E), BF16), V((ROWS, E), F32), V((ROWS, E), F32), V((ROWS, E), F32), V((ROWS, E), F32),
            V((ROWS, 128), F32), V((2, N, 8, E), F32),
            V((2, PW, HR), F32), V((2, 2, PH, HR), BF16), V((2, 2, PH, HR), BF16), V((2, 2, PH, HR), BF16), V((2, 2, 3, PH, HR), BF16),
            V((2, 2, PW, HR), F32),
            V((NCH, CR, HALF), F32), V((NCH, CR, HALF), BF16), V((2, NCH, CR, HALF), BF16), V((NCH, CR, HALF), BF16),
            V((2, NCH, CR, HALF), BF16), V((NCH, CR, HALF), BF16), V((2, NCH, CR, HALF), BF16), V((2, 2, NCH, CR, HALF), BF16),
            dma((8,)), dma((HC,)), dma((2, KB)), dma((4,)), dma((2,)), dma((2,)),
            dma((2,)), dma((2,)), dma((2, 3)), dma((2, 3)), dma((2,)), dma((2,)),
        ] + [dma, dma((NCH,))] * 5
        resid, conv_out, ssm = pl.pallas_call(
            body,
            out_shape=(V((ROWS, D), F32), V((2, 3, ROWS, E), BF16), V((2, N, ROWS, E), F32)),
            in_specs=[hbm] * 13,
            out_specs=(vmem, vmem, vmem),
            scratch_shapes=scratch,
            compiler_params=pltpu.CompilerParams(collective_id=0, has_side_effects=True, vmem_limit_bytes=43 * 1024 * 1024),
        )(residual, norm_w, w_rows, conv_w, conv_b, w_xt, w_dt, b_dt, a_log, d_skip, w_out, conv_t, ssm_state)
        resid, conv_out, ssm = (pltpu.with_memory_space_constraint(v, V) for v in (resid, conv_out, ssm))
        resid, conv_out, ssm = pl.pallas_call(
            write_out,
            out_shape=[jax.ShapeDtypeStruct(v.shape, v.dtype) for v in (resid, conv_out, ssm_state)],
            in_specs=[vmem] * 3,
            out_specs=[hbm] * 3,
            scratch_shapes=[dma((3,))],
            compiler_params=pltpu.CompilerParams(vmem_limit_bytes=24 * 1024 * 1024),
        )(resid, conv_out, ssm)
        return resid, jnp.transpose(conv_out, (0, 2, 1, 3)), ssm

    cache_spec = P(None, 'dp', None, 'tp')
    in_specs = (P('dp', None), P(None, None), P(None, None, None, 'tp'), P(None, None, 'tp'), P(None, 'tp'), P(None, 'tp', None), P(None, None, 'tp'), P(None, 'tp'), P(None, None, 'tp'), P(None, 'tp'), P(None, 'tp', None), cache_spec, cache_spec)
    out_specs = (P('dp', None), cache_spec, cache_spec)
    return jax.shard_map(device_step, mesh=mesh, in_specs=in_specs, out_specs=out_specs, check_vma=False)
```

```python
import functools

import jax
import jax.numpy as jnp
from jax import lax
from jax.experimental import pallas as pl
from jax.experimental.pallas import tpu as pltpu
from jax.sharding import PartitionSpec as P

MESH = pl.DeviceIdType.MESH
LOG2E = 1.4426950408889634
F32, BF16 = jnp.float32, jnp.bfloat16

ROWS = 256
D = 2048
E = 512
N = 16
RANK = 128
PW = RANK + 2 * N
NCH = 8
CR = ROWS // NCH
HALF = D // 2
KB = 8
KD = D // KB
HR = ROWS // 2
HC = NCH // 2
PH = PW // 2
FIRST = 3
OFF_B, OFF_C, OFF_D, OFF_E, OFF_F = 1, 4, 7, 10, 11
T_FRONT = HC - 1 + OFF_F
P_WAIT = 4
NEXT = T_FRONT + P_WAIT + 1


def silu(v):
    return v * jax.nn.sigmoid(v)


def rms(v, axis, eps):
    return v * lax.rsqrt(jnp.mean(v * v, axis=axis, keepdims=True) + eps)


def body(
    resid_in, norm_w, w_in, conv_w, conv_b, w_xt, w_dt, b_dt, a_log, d_skip, w_out, conv_in, ssm_in,
    resid, conv_out, ssm,
    v_norm, v_convw, v_convb, v_wxt, v_wdt, v_bdt, v_alog, v_dskip,
    w_raw, w_xz, s32, v_wout, conv0,
    hid, xcb, gate, dtb, dtx, dsx, bcb, a2,
    p_own, p_sa, p_ra, p_sb, p_rb, p_full,
    own, o_sa, o_ra, o_sb, o_rb, o_sc, o_rc, tot,
    small_sem, resid_sem, win_sem, conv_sem, ssm_sem, wout_sem,
    pa_send, pa_recv, pb_send, pb_recv, pf_send, pf_recv,
    a_send, a_recv, b_send, b_recv, c_send, c_recv, t_send, t_recv, f_send, f_recv,
):
    dp = lax.axis_index("dp")
    me = lax.axis_index("tp")
    core = lax.rem(me, 2)
    z = me // 2
    is_end = (z == 0) | (z == 3)
    is_mid = (z == 1) | (z == 2)
    partner = me + 1 - 2 * core
    zodd = lax.rem(z, 2)
    zpair = me + 2 - 4 * zodd
    midpeer = (3 - z) * 2 + core

    def dev(t):
        return (dp, t)

    def remote(src, dst, ssem, rsem, target):
        return pltpu.make_async_remote_copy(
            src_ref=src, dst_ref=dst, send_sem=ssem, recv_sem=rsem, device_id=dev(target), device_id_type=MESH)

    barrier = pltpu.get_barrier_semaphore()
    pl.semaphore_signal(barrier, inc=1, device_id=dev(partner), device_id_type=MESH)
    for k in range(1, 4):
        pl.semaphore_signal(barrier, inc=1, device_id=dev(lax.rem(me + 2 * k, 8)), device_id_type=MESH)

    copies = {}

    def load(key, src, dst, sem):
        c = pltpu.make_async_copy(src, dst, sem)
        c.start()
        copies[key] = c

    def wait(key):
        copies.pop(key).wait()

    def load_win(l, blocks):
        for kb in blocks:
            rows = pl.ds(kb * 8 * KD, 8 * KD)
            load(("win", l, kb), w_in.at[l, rows], w_raw.at[l, rows], win_sem.at[l, kb])

    def load_conv(l):
        load(("conv0", l), conv_in.at[l, 0], conv0.at[l], conv_sem.at[2 * l])
        load(("conv", l), conv_in.at[l, pl.ds(1, 2)], conv_out.at[l, pl.ds(0, 2)], conv_sem.at[2 * l + 1])

    def load_state(l):
        load(("wout", l), w_out.at[l], v_wout.at[l], wout_sem.at[l])
        for n in range(N):
            load_plane(l, n)

    def load_plane(l, n):
        pltpu.make_async_copy(ssm_in.at[l, :, n, :], ssm.at[l, n], ssm_sem.at[l]).start()

    def wait_planes(l):
        pltpu.make_async_copy(ssm.at[l], ssm.at[l], ssm_sem.at[l]).wait()

    load("norm", norm_w, v_norm, small_sem.at[0])
    load_win(0, range(FIRST))
    for i in range(HC):
        rows = pl.ds(i * 2 * CR, 2 * CR)
        load(("resid", i), resid_in.at[rows], resid.at[rows], resid_sem.at[i])
    load_win(0, range(FIRST, KB))
    small = ((conv_w, v_convw), (conv_b, v_convb), (w_xt, v_wxt), (w_dt, v_wdt), (b_dt, v_bdt), (a_log, v_alog), (d_skip, v_dskip))
    for i, (s, d) in enumerate(small):
        load(("small", i), s, d, small_sem.at[i + 1])
    load_conv(0)

    def row_of(ref, l):
        v = ref[...].astype(F32)
        return jnp.where(l == 0, v[0:1, :], v[1:2, :])

    def unpack(l, kb):
        s32[kb] = w_raw[l, pl.ds(pl.multiple_of(kb * 8 * KD, 8 * KD), 8 * KD), :].astype(F32)

    def pack(kb):
        rows = pl.ds(pl.multiple_of(kb * KD, KD), KD)
        for w in range(2):
            for j in range(4):
                w_xz[w, rows, j * 128:(j + 1) * 128] = s32[kb, pl.ds(2 * j + w, KD, stride=8), :].astype(BF16)

    def normed(l, i):
        rows = pl.ds(pl.multiple_of(i * CR, CR), CR)
        hid[rows, :] = (rms(resid[rows, :], 1, 1e-5) * row_of(v_norm, l)).astype(BF16)

    def front(l, h):
        rows = pl.ds(pl.multiple_of(h * HR, HR), HR)
        x_b = jnp.dot(hid[rows, :], w_xz[0], preferred_element_type=F32).astype(BF16)
        conv_out[l, 2, rows, :] = x_b
        gate[rows, :] = silu(jnp.dot(hid[rows, :], w_xz[1], preferred_element_type=F32).astype(BF16).astype(F32))
        cw = v_convw[l].astype(F32)
        pre = row_of(v_convb, l) + cw[3:4, :] * conv_out[l, 2, rows, :].astype(F32)
        pre = pre + cw[0:1, :] * conv0[l, rows, :].astype(F32)
        pre = pre + cw[1:2, :] * conv_out[l, 0, rows, :].astype(F32)
        pre = pre + cw[2:3, :] * conv_out[l, 1, rows, :].astype(F32)
        xcb[rows, :] = silu(pre).astype(BF16)
        dsx[rows, :] = row_of(v_dskip, l) * xcb[rows, :].astype(F32)
        p_own[h] = lax.dot_general(v_wxt[l], xcb[rows, :], (((1,), (1,)), ((), ())), preferred_element_type=F32)

    mine = pl.ds(pl.multiple_of(core * PH, PH), PH)
    theirs = pl.ds(pl.multiple_of((1 - core) * PH, PH), PH)

    def copy_pa(l, h):
        return remote(p_sa.at[l, h], p_ra.at[l, h], pa_send.at[h], pa_recv.at[h], partner)

    def copy_pb(l, h, k):
        return remote(p_sb.at[l, h], p_rb.at[l, h, k - 1], pb_send.at[h, k - 1], pb_recv.at[h, k - 1], lax.rem(me + 2 * k, 8))

    def copy_pf(l, h):
        return remote(p_full.at[l, h, mine], p_full.at[l, h, mine], pf_send.at[h], pf_recv.at[h], partner)

    def p_one(l, h):
        p_sa[l, h] = p_own[h, theirs, :].astype(BF16)
        copy_pa(l, h).start()

    def p_two(l, h):
        copy_pa(l, h).wait_recv()
        p_sb[l, h] = (p_own[h, mine, :] + p_ra[l, h].astype(F32)).astype(BF16)
        for k in range(1, 4):
            copy_pb(l, h, k).start()

    def p_three(l, h):
        for k in range(1, 4):
            copy_pb(l, h, k).wait_recv()
        total = jnp.zeros((PH, HR), F32)
        parts = [p_sb[l, h].astype(F32)] + [p_rb[l, h, k].astype(F32) for k in range(3)]
        for chip in range(4):
            d = lax.rem(z - chip + 4, 4)
            total = total + jnp.where(d == 0, parts[0], jnp.where(d == 1, parts[1], jnp.where(d == 2, parts[2], parts[3])))
        p_full[l, h, mine, :] = total
        copy_pf(l, h).start()

    def p_left(l, h):
        copy_pa(l, h).wait_send()
        for k in range(1, 4):
            copy_pb(l, h, k).wait_send()
        copy_pf(l, h).wait_send()

    def rates(l):
        for n in range(N):
            a2[l, n] = jnp.broadcast_to(-jnp.exp(v_alog[l, n:n + 1, :]) * LOG2E, (8, E))

    def p_four(l, h):
        copy_pf(l, h).wait_recv()
        rows = pl.ds(pl.multiple_of(h * HR, HR), HR)
        pt = p_full[l, h]
        low = rms(pt[:RANK].T, 1, 1e-6).astype(BF16)
        lin = jnp.dot(low, v_wdt[l], preferred_element_type=F32) + row_of(v_bdt, l)
        dt = jnp.maximum(lin, 0.0) + jnp.log1p(jnp.exp(-jnp.abs(lin)))
        dtb[rows, :] = dt
        dtx[rows, :] = dt * xcb[rows, :].astype(F32)
        b = rms(pt[RANK:RANK + N], 0, 1e-6)
        c = rms(pt[RANK + N:], 0, 1e-6)
        bc = jnp.concatenate([b, c, jnp.zeros((128 - 2 * N, HR), F32)], axis=0)
        bcb[rows, :] = bc.T

    def stage_a(l, i):
        r0 = pl.multiple_of(i * CR, CR)

        rows = pl.ds(r0, CR)
        bc = bcb[rows, :]
        dt = dtb[rows, :]
        dx = dtx[rows, :]
        y = dsx[rows, :]
        for n in range(N):
            rate = jnp.concatenate([a2[l, n]] * (CR // 8), axis=0)
            new = jnp.exp2(dt * rate) * ssm[l, n, rows, :] + dx * bc[:, n:n + 1]
            ssm[l, n, rows, :] = new
            y = y + new * bc[:, N + n:N + n + 1]
        yg = (y * gate[rows, :]).astype(BF16)
        their_cols = pl.ds(pl.multiple_of((1 - core) * HALF, HALF), HALF)
        our_cols = pl.ds(pl.multiple_of(core * HALF, HALF), HALF)
        o_sa[i] = jnp.dot(yg, v_wout[l, :, their_cols], preferred_element_type=F32).astype(BF16)
        copy_a(l, i).start()
        own[i] = jnp.dot(yg, v_wout[l, :, our_cols], preferred_element_type=F32)

    def copy_a(l, i):
        return remote(o_sa.at[i], o_ra.at[l, i], a_send, a_recv.at[i], partner)

    def copy_b(l, i):
        return remote(o_sb.at[i], o_rb.at[l, i], b_send, b_recv.at[i], zpair)

    def copy_c(l, i):
        return remote(o_sc.at[i], o_rc.at[l, i], c_send, c_recv.at[i], midpeer)

    def copy_t(l, i):
        return remote(tot.at[l, core, i], tot.at[l, core, i], t_send, t_recv.at[i], zpair)

    def copy_f(l, i):
        return remote(tot.at[l, core, i], tot.at[l, core, i], f_send, f_recv.at[i], partner)

    def stage_b(l, i):
        copy_a(l, i).wait_recv()
        chip = own[i] + o_ra[l, i].astype(F32)

        @pl.when(is_end)
        def _():
            o_sb[i] = chip.astype(BF16)
            copy_b(l, i).start()

        @pl.when(is_mid)
        def _():
            own[i] = chip

    def stage_c(l, i):
        @pl.when(is_mid)
        def _():
            copy_b(l, i).wait_recv()
            o_sc[i] = (own[i] + o_rb[l, i].astype(F32)).astype(BF16)
            copy_c(l, i).start()

    def stage_d(l, i):
        @pl.when(is_mid)
        def _():
            copy_c(l, i).wait_recv()
            tot[l, core, i] = (o_sc[i].astype(F32) + o_rc[l, i].astype(F32)).astype(BF16)
            copy_t(l, i).start()
            copy_f(l, i).start()

    def stage_e(l, i):
        @pl.when(is_end)
        def _():
            copy_t(l, i).wait_recv()
            copy_f(l, i).start()

    def stage_f(l, i):
        copy_f(l, i).wait_recv()
        rows = pl.ds(pl.multiple_of(i * CR, CR), CR)
        resid[rows, :HALF] = resid[rows, :HALF] + tot[l, 0, i].astype(F32)
        resid[rows, HALF:] = resid[rows, HALF:] + tot[l, 1, i].astype(F32)

        @pl.when(l == 0)
        def _():
            normed(1, i)

    def o_left(l):
        remote(o_sa, o_sa, a_send, a_recv.at[0], partner).wait_send()
        remote(tot.at[l, core], tot.at[l, core], f_send, f_recv.at[0], partner).wait_send()

        @pl.when(is_end)
        def _():
            remote(o_sb, o_sb, b_send, b_recv.at[0], zpair).wait_send()

        @pl.when(is_mid)
        def _():
            remote(o_sc, o_sc, c_send, c_recv.at[0], midpeer).wait_send()
            remote(tot.at[l, core], tot.at[l, core], t_send, t_recv.at[0], zpair).wait_send()

    for kb in range(KB):
        if kb == FIRST:
            wait("norm")
            for i in range(HC):
                wait(("resid", i))
                normed(0, 2 * i)
                normed(0, 2 * i + 1)
            load_state(0)
            load_win(1, range(KB))
        wait(("win", 0, kb))
        unpack(0, kb)
        if kb > 0:
            pack(kb - 1)
    pack(KB - 1)
    for i in range(len(small)):
        wait(("small", i))
    wait(("conv0", 0))
    wait(("conv", 0))

    def first(h, c):
        front(0, h)

        @pl.when(h == 0)
        def _():
            pl.semaphore_wait(barrier, 4)

        p_one(0, h)
        return c

    lax.fori_loop(0, 2, first, 0)
    p_two(0, 0)
    rates(0)
    rates(1)
    for kb in range(KB):
        wait(("win", 1, kb))

    def unpack_next(kb, c):
        unpack(1, kb)
        return c

    def pack_next(kb, c):
        pack(kb)
        return c

    lax.fori_loop(0, KB, unpack_next, 0)
    p_two(0, 1)
    lax.fori_loop(0, KB, pack_next, 0)
    p_three(0, 0)
    wait(("wout", 0))
    wait_planes(0)
    load_conv(1)
    load(("wout", 1), w_out.at[1], v_wout.at[1], wout_sem.at[1])
    p_four(0, 0)

    def step(t, c):
        def chunks(off, stage):
            v = t - off
            l = jnp.where(v >= NEXT, 1, 0)
            i = v - NEXT * l

            @pl.when((v >= 0) & (i < NCH))
            def _():
                stage(l, i)

        def halves(at, stage, first_at=None):
            h = jnp.where(t == at, 0, 1)
            l = jnp.where(t >= at, 1, 0)
            now = (t == at) | (t == at + HC)
            if first_at is not None:
                now = now | (t == first_at)

            @pl.when(now)
            def _():
                stage(l, h)

        def enter(l, h):
            front(l, h)
            p_one(l, h)

        @pl.when(t < N)
        def _():
            load_plane(1, t)

        @pl.when(t == T_FRONT)
        def _():
            for h in range(2):
                p_left(0, h)
            for key in (("wout", 1), ("conv0", 1), ("conv", 1)):
                wait(key)

        @pl.when(t == NEXT)
        def _():
            wait_planes(1)
            o_left(0)

        halves(NEXT, p_four, HC)
        chunks(0, stage_a)
        chunks(OFF_B, stage_b)
        chunks(OFF_D, stage_d)
        chunks(OFF_C, stage_c)
        halves(T_FRONT + 1, p_two)
        chunks(OFF_E, stage_e)
        chunks(OFF_F, stage_f)
        halves(T_FRONT, enter)
        halves(T_FRONT + P_WAIT, p_three, 2)
        return c

    lax.fori_loop(0, NEXT + NCH + OFF_F, step, 0)
    o_left(1)
    for h in range(2):
        p_left(1, h)


def write_out(resid, conv, ssm, resid_out, conv_out, ssm_out, sem):
    for l in range(2):
        for n in range(N):
            pltpu.make_async_copy(ssm.at[l, n], ssm_out.at[l, :, n, :], sem.at[0]).start()
    others = [pltpu.make_async_copy(resid, resid_out, sem.at[1]), pltpu.make_async_copy(conv, conv_out, sem.at[2])]
    for c in others:
        c.start()
    for c in others:
        c.wait()
    pltpu.make_async_copy(ssm, ssm, sem.at[0]).wait()


def solution(mesh):
    hbm = pl.BlockSpec(memory_space=pl.ANY)
    vmem = pl.BlockSpec(memory_space=pltpu.VMEM)
    V = pltpu.VMEM
    dma = pltpu.SemaphoreType.DMA

    def device_step(residual, norm_w, w_in, conv_w, conv_b, w_x, w_dt, b_dt, a_log, d_skip, w_out, conv_state, ssm_state):
        conv_t = jnp.transpose(conv_state, (0, 2, 1, 3))
        w_xt = jnp.transpose(w_x, (0, 2, 1))
        w_rows = jnp.transpose(w_in.reshape(2, D, 2, 4, 128), (0, 1, 3, 2, 4)).reshape(2, 8 * D, 128)
        scratch = [
            V((2, D), BF16), V((2, 4, E), BF16), V((2, E), BF16), V((2, PW, E), BF16), V((2, RANK, E), BF16),
            V((2, E), F32), V((2, N, E), F32), V((2, E), F32),
            V((2, 8 * D, 128), BF16), V((2, D, E), BF16), V((KB, 8 * KD, 128), F32), V((2, E, D), BF16), V((2, ROWS, E), BF16),
            V((ROWS, D), BF16), V((ROWS, E), BF16), V((ROWS, E), F32), V((ROWS, E), F32), V((ROWS, E), F32), V((ROWS, E), F32),
            V((ROWS, 128), F32), V((2, N, 8, E), F32),
            V((2, PW, HR), F32), V((2, 2, PH, HR), BF16), V((2, 2, PH, HR), BF16), V((2, 2, PH, HR), BF16), V((2, 2, 3, PH, HR), BF16),
            V((2, 2, PW, HR), F32),
            V((NCH, CR, HALF), F32), V((NCH, CR, HALF), BF16), V((2, NCH, CR, HALF), BF16), V((NCH, CR, HALF), BF16),
            V((2, NCH, CR, HALF), BF16), V((NCH, CR, HALF), BF16), V((2, NCH, CR, HALF), BF16), V((2, 2, NCH, CR, HALF), BF16),
            dma((8,)), dma((HC,)), dma((2, KB)), dma((4,)), dma((2,)), dma((2,)),
            dma((2,)), dma((2,)), dma((2, 3)), dma((2, 3)), dma((2,)), dma((2,)),
        ] + [dma, dma((NCH,))] * 5
        resid, conv_out, ssm = pl.pallas_call(
            body,
            out_shape=(V((ROWS, D), F32), V((2, 3, ROWS, E), BF16), V((2, N, ROWS, E), F32)),
            in_specs=[hbm] * 13,
            out_specs=(vmem, vmem, vmem),
            scratch_shapes=scratch,
            compiler_params=pltpu.CompilerParams(collective_id=0, has_side_effects=True, vmem_limit_bytes=43 * 1024 * 1024),
        )(residual, norm_w, w_rows, conv_w, conv_b, w_xt, w_dt, b_dt, a_log, d_skip, w_out, conv_t, ssm_state)
        resid, conv_out, ssm = (pltpu.with_memory_space_constraint(v, V) for v in (resid, conv_out, ssm))
        resid, conv_out, ssm = pl.pallas_call(
            write_out,
            out_shape=[jax.ShapeDtypeStruct(v.shape, v.dtype) for v in (resid, conv_out, ssm_state)],
            in_specs=[vmem] * 3,
            out_specs=[hbm] * 3,
            scratch_shapes=[dma((3,))],
            compiler_params=pltpu.CompilerParams(vmem_limit_bytes=24 * 1024 * 1024),
        )(resid, conv_out, ssm)
        return resid, jnp.transpose(conv_out, (0, 2, 1, 3)), ssm

    cache_spec = P(None, 'dp', None, 'tp')
    in_specs = (P('dp', None), P(None, None), P(None, None, None, 'tp'), P(None, None, 'tp'), P(None, 'tp'), P(None, 'tp', None), P(None, None, 'tp'), P(None, 'tp'), P(None, None, 'tp'), P(None, 'tp'), P(None, 'tp', None), cache_spec, cache_spec)
    out_specs = (P('dp', None), cache_spec, cache_spec)
    return jax.shard_map(device_step, mesh=mesh, in_specs=in_specs, out_specs=out_specs, check_vma=False)
```
